256 devices in a mesh: gx: 4 (over x), gy: 8 (over z), gz: 8 (over y, core).
Axes of the slice: x: 4, y: 4, z: 8, core: 2. Of those that a mesh axis runs over, the one named last changes fastest.
Arguments:
- viscosity: float32 [128, 128, 1024], P('gx', 'gy', 'gz'), may hold values from 0.001 to 1000
- force: float32 [3, 128, 128, 1024], P(None, 'gx', 'gy', 'gz'), may hold values from -6 to 6
Outputs:
- solution: float32 [4, 128, 128, 1024], P(None, 'gx', 'gy', 'gz')
- residual: float32 [4, 128, 128, 1024], P(None, 'gx', 'gy', 'gz')
The draws below stay inside these ranges and needn't reach their ends.
All inputs are finite; a program needn't handle non-finite values.
Results may differ from the reference program's by a relative error of at most 0.0003.
Values sent between devices are 32-bit elements; how exact they have to be, the bound alone decides.
No kernel may reach another device: no remote copies, remote signals or barrier semaphores. Data moves between devices by JAX's collectives and lax.ppermute only.
A program may use at most 128 MiB of HBM per device.

```python
import math
import jax
import jax.numpy as jnp
from jax import lax

CHEB = 4
ITERS = 2
NX = 128
NY = 128
NZ = 1024


def steps_of(rng, dims, pieces, low, largest):
    level = 1.0
    for dim, shards_of in pieces:
        draws = jax.random.uniform(jax.random.fold_in(jax.random.fold_in(rng, 6), dim), (shards_of,), jnp.float32, low / len(pieces), largest / len(pieces))
        level = level * jnp.repeat(jnp.exp(draws), dims[dim] // shards_of).reshape((-1,) + (1,) * (len(dims) - 1 - dim))
    return level


def scatter_about(own_key, dims, deviation, bound, cuts=(), kind=jnp.bfloat16):
    values = deviation * jax.random.normal(own_key, dims, jnp.float32)
    if cuts:
        values = values * steps_of(own_key, dims, cuts, -0.22, 0.18)
    return jnp.clip(values, -bound, bound).astype(kind)


def setup_inputs(seed: int = 0) -> dict:
    splits = jax.random.split(jax.random.key(seed), 3)
    viscosity = jnp.clip(jnp.exp(math.log(1000.0) - 13.815511 * jax.random.uniform(splits[0], (NX, NY, NZ), jnp.float32) ** steps_of(splits[0], (NX, NY, NZ), ((0, 4), (1, 8), (2, 8)), -0.2, 0.2)), 0.001, 1000.0)
    force = scatter_about(splits[1], (3, NX, NY, NZ), 1.0, 6.0, ((1, 4), (2, 8), (3, 8)), jnp.float32)
    return dict(viscosity=viscosity, force=force)


low_edge = 0.25
high_edge = 2.0

def coefficients(padded_eta):
    middle = padded_eta[1:-1, 1:-1, 1:-1]
    x_plus = 0.5 * (middle + padded_eta[2:, 1:-1, 1:-1])
    x_minus = 0.5 * (middle + padded_eta[:-2, 1:-1, 1:-1])
    y_plus = 0.5 * (middle + padded_eta[1:-1, 2:, 1:-1])
    y_minus = 0.5 * (middle + padded_eta[1:-1, :-2, 1:-1])
    z_plus = 0.5 * (middle + padded_eta[1:-1, 1:-1, 2:])
    z_minus = 0.5 * (middle + padded_eta[1:-1, 1:-1, :-2])
    diagonal = x_plus + x_minus + y_plus + y_minus + z_plus + z_minus
    return (x_plus, x_minus, y_plus, y_minus, z_plus, z_minus, diagonal)

def viscous(padded, stencil):
    x_plus, x_minus, y_plus, y_minus, z_plus, z_minus, diagonal = stencil
    result = diagonal * padded[:, 1:-1, 1:-1, 1:-1]
    result = result - x_plus * padded[:, 2:, 1:-1, 1:-1] - x_minus * padded[:, :-2, 1:-1, 1:-1]
    result = result - y_plus * padded[:, 1:-1, 2:, 1:-1] - y_minus * padded[:, 1:-1, :-2, 1:-1]
    result = result - z_plus * padded[:, 1:-1, 1:-1, 2:] - z_minus * padded[:, 1:-1, 1:-1, :-2]
    return result

def stokes(padded, stencil):
    velocity = padded[:3]
    pressure = padded[3]
    gradient = jnp.stack([0.5 * (pressure[2:, 1:-1, 1:-1] - pressure[:-2, 1:-1, 1:-1]), 0.5 * (pressure[1:-1, 2:, 1:-1] - pressure[1:-1, :-2, 1:-1]), 0.5 * (pressure[1:-1, 1:-1, 2:] - pressure[1:-1, 1:-1, :-2])])
    divergence = -0.5 * (velocity[0, 2:, 1:-1, 1:-1] - velocity[0, :-2, 1:-1, 1:-1] + (velocity[1, 1:-1, 2:, 1:-1] - velocity[1, 1:-1, :-2, 1:-1]) + (velocity[2, 1:-1, 1:-1, 2:] - velocity[2, 1:-1, 1:-1, :-2]))
    return jnp.concatenate([viscous(velocity, stencil) + gradient, divergence[None]], axis=0)

def pad_cells(field):
    return jnp.pad(field, ((0, 0), (1, 1), (1, 1), (1, 1)))

def chebyshev(forcing, inverse, apply_block):
    middle = 0.5 * (high_edge + low_edge)
    half_width = 0.5 * (high_edge - low_edge)
    scaled = middle / half_width
    ratio_now = 1.0 / scaled
    update = forcing * inverse / middle
    result = update
    remainder = forcing
    for sweep_at in range(CHEB - 1):
        remainder = remainder - apply_block(update)
        ratio_next = 1.0 / (2.0 * scaled - ratio_now)
        update = ratio_next * ratio_now * update + 2.0 * ratio_next / half_width * remainder * inverse
        result = result + update
        ratio_now = ratio_next
    return result

def least_squares(columns, initial_norm):
    hessen = jnp.stack(columns, axis=1)
    normal = jnp.dot(hessen.T, hessen, precision=lax.Precision.HIGHEST)
    target = initial_norm * hessen[0]
    factor = jnp.linalg.cholesky(normal)
    size_of = len(columns)
    forward = []
    for row_at in range(size_of):
        running = target[row_at]
        for inner_at in range(row_at):
            running = running - factor[row_at, inner_at] * forward[inner_at]
        forward.append(running / factor[row_at, row_at])
    backward = [None] * size_of
    for row_at in reversed(range(size_of)):
        running = forward[row_at]
        for inner_at in range(row_at + 1, size_of):
            running = running - factor[inner_at, row_at] * backward[inner_at]
        backward[row_at] = running / factor[row_at, row_at]
    weights = jnp.stack(backward)
    leading = jnp.zeros((size_of + 1,), jnp.float32).at[0].set(initial_norm)
    misfit = leading - jnp.dot(hessen, weights, precision=lax.Precision.HIGHEST)
    return (backward, misfit)

def reference(viscosity, force):
    stencil = coefficients(jnp.pad(viscosity, 1))
    inverse = 1.0 / stencil[6]

    def velocity_block(update):
        return viscous(pad_cells(update), stencil)
    rhs_full = jnp.concatenate([force, jnp.zeros((1,) + viscosity.shape, jnp.float32)], axis=0)
    initial_norm = jnp.sqrt(jnp.sum(rhs_full * rhs_full))
    krylov = [rhs_full / initial_norm]
    search = []
    columns = []
    for column_at in range(ITERS):
        current = krylov[column_at]
        smoothed = chebyshev(current[:3], inverse, velocity_block)
        direction = jnp.concatenate([smoothed, (viscosity * current[3])[None]], axis=0)
        search.append(direction)
        candidate = stokes(pad_cells(direction), stencil)
        products = jnp.stack([jnp.sum(candidate * vector) for vector in krylov])
        for row_at in range(column_at + 1):
            candidate = candidate - products[row_at] * krylov[row_at]
        length = jnp.sqrt(jnp.sum(candidate * candidate))
        krylov.append(candidate / length)
        columns.append(jnp.concatenate([products, length[None], jnp.zeros((ITERS - 1 - column_at,), jnp.float32)]))
    weights, misfit = least_squares(columns, initial_norm)
    solution = weights[0] * search[0]
    for column_at in range(1, ITERS):
        solution = solution + weights[column_at] * search[column_at]
    residual = misfit[0] * krylov[0]
    for row_at in range(1, ITERS + 1):
        residual = residual + misfit[row_at] * krylov[row_at]
    return (solution, residual)
```

```python
import functools

import jax
import jax.numpy as jnp
from jax import lax
from jax.experimental import pallas as pl
from jax.experimental.pallas import tpu as pltpu
from jax.sharding import PartitionSpec as P

CHEB = 4
LOW_EDGE = 0.25
HIGH_EDGE = 2.0
MIDDLE = 0.5 * (HIGH_EDGE + LOW_EDGE)
HALF = 0.5 * (HIGH_EDGE - LOW_EDGE)
AXES = ("gx", "gy", "gz")

BX, BY, BZ, H = 32, 16, 128, 8
EX, EY, EZ = BX + 2 * H, BY + 2 * H, BZ + 2 * H
CHUNKS = 4
SLABS = EX // CHUNKS
LANES = CHUNKS * EY
ROWS = EZ + 16
YTILES = 4 * EX + BX // 8
ZTILES = 4 * SLABS + 2
OWN = slice(16, 16 + BZ)
PIECES = [(8, 8)] + [(16 + 16 * i, 16) for i in range(8)] + [(144, 8)]
OWN_PIECES = PIECES[1:-1]


def chebyshev_factors():
    scaled = MIDDLE / HALF
    now = 1.0 / scaled
    pairs = []
    for _ in range(CHEB - 1):
        following = 1.0 / (2.0 * scaled - now)
        pairs.append((following * now, 2.0 * following / HALF))
        now = following
    return pairs


def pack_y(force, visc, low_x, high_x, tail, head):
    for out, first in ((tail, BY - 8), (head, 0)):
        rows = slice(first, first + 8)
        for c in range(3):
            base = c * EX
            out[base : base + 8] = low_x[c * 8 : c * 8 + 8, rows, :]
            out[base + 8 : base + 8 + BX] = force[c, :, rows, :]
            out[base + 8 + BX : base + EX] = high_x[c * 8 : c * 8 + 8, rows, :]
        base = 3 * EX
        out[base : base + 8] = low_x[25:33, rows, :]
        out[base + 8 : base + 8 + BX] = visc[:, rows, :]
        out[base + 8 + BX : base + EX] = high_x[24:32, rows, :]
        ninth = first - 1 if first else 8
        for x in range(BX):
            out[4 * EX + x // 8, x % 8, :] = visc[x, ninth, :]


def to_lanes(force, visc, low_x, high_x, low_y, high_y, f_out, v_out, ry_out, ex_out, tail, head):
    def rows_of(c, at):
        x = at - H
        if x < 0:
            middle = low_x[c * 8 + at] if c < 3 else low_x[25 + at]
        elif x >= BX:
            middle = high_x[c * 8 + x - BX] if c < 3 else high_x[24 + x - BX]
        else:
            middle = force[c, x] if c < 3 else visc[x]
        return [low_y[c * EX + at], middle, high_y[c * EX + at]]

    for c in range(4):
        for g in range(SLABS):
            parts = []
            for k in range(CHUNKS):
                parts += rows_of(c, k * SLABS + g)
            block = jnp.concatenate(parts, axis=0).T
            if c < 3:
                f_out[c, g] = block
            else:
                v_out[g] = block
                tail[4 * SLABS + g // 8, g % 8 : g % 8 + 1, :] = block[BZ - 9 : BZ - 8]
                head[4 * SLABS + g // 8, g % 8 : g % 8 + 1, :] = block[8:9]
            tail[c * SLABS + g] = block[BZ - 8 :]
            head[c * SLABS + g] = block[:8]
    for out in (tail, head):
        out[ZTILES - 1, SLABS - 8 :, :] = jnp.zeros((16 - SLABS, LANES), jnp.float32)
    nothing = jnp.zeros((EY - 2, BZ), jnp.float32)
    for g in range(SLABS):
        parts = []
        for k in range(CHUNKS):
            x = k * SLABS + g - H
            if 0 <= x < BX:
                at = 4 * EX + x // 8
                lower, upper = low_y[at, x % 8 : x % 8 + 1, :], high_y[at, x % 8 : x % 8 + 1, :]
            else:
                lower = upper = jnp.zeros((1, BZ), jnp.float32)
            parts += [lower, nothing, upper]
        ry_out[g] = jnp.concatenate(parts, axis=0).T
    side = jnp.zeros((8, BZ), jnp.float32)
    between = jnp.zeros((2 * EY, BZ), jnp.float32)
    ex_out[...] = jnp.concatenate(
        [side, low_x[24], side, between, side, high_x[32], side], axis=0
    ).T


def lane_index(rows):
    return lax.broadcasted_iota(jnp.int32, (rows, LANES), 1)


def solve_local(
    f, v, ry, ex, low_z, high_z,
    s0_out, u1_out, s1_out, u2_out, sums,
    visc, coef, inv, diag, d0, d1, d2, s, r, p,
):
    def place(g, _):
        visc[g + 1, 0:8] = jnp.zeros((8, LANES), jnp.float32)
        visc[g + 1, 152:160] = jnp.zeros((8, LANES), jnp.float32)
        visc[g + 1, 8:16] = low_z[3 * SLABS + g]
        visc[g + 1, OWN] = v[g]
        visc[g + 1, 144:152] = high_z[3 * SLABS + g]
        return 0

    lax.fori_loop(0, SLABS, place, 0)
    for g in range(SLABS):
        visc[g + 1, 7:8] = low_z[4 * SLABS + g // 8, g % 8 : g % 8 + 1, :]
        visc[g + 1, 152:153] = high_z[4 * SLABS + g // 8, g % 8 : g % 8 + 1, :]
    for first, count in PIECES:
        rows = slice(first, first + count)
        before = pltpu.roll(visc[SLABS, rows], EY, 1)
        after = pltpu.roll(visc[1, rows], LANES - EY, 1)
        if 16 <= first < 144:
            lane = lane_index(count)
            extra = ex[first - 16 : first - 16 + count]
            before = jnp.where(lane < EY, extra, before)
            after = jnp.where(lane >= LANES - EY, extra, after)
        visc[0, rows] = before
        visc[SLABS + 1, rows] = after

    def border(ref, which):
        zero = jnp.zeros((8, LANES), jnp.float32)
        for c in which:
            for g in range(SLABS):
                at = (c, g + 1) if c is not None else (g + 1,)
                ref[(*at, slice(0, 8))] = zero
                ref[(*at, slice(152, 160))] = zero

    for ref in (d0, d1, d2, s):
        border(ref, range(3))
    border(p, [None])

    def ghosts(ref, which):
        for c in which:
            for first, count in PIECES:
                rows = slice(first, first + count)
                pre = (c,) if c is not None else ()
                ref[(*pre, 0, rows)] = pltpu.roll(ref[(*pre, SLABS, rows)], EY, 1)
                ref[(*pre, SLABS + 1, rows)] = pltpu.roll(ref[(*pre, 1, rows)], LANES - EY, 1)

    def setup(g, _):
        at = g + 1
        for first, count in PIECES:
            rows = slice(first, first + count)
            here = slice(first - 8, first - 8 + count)
            lane = lane_index(count)
            y_at = lane & (EY - 1)
            mine = visc[at, rows]
            below, above = pltpu.roll(mine, 1, 1), pltpu.roll(mine, LANES - 1, 1)
            if 16 <= first < 144:
                extra = ry[g, first - 16 : first - 16 + count]
                below = jnp.where(y_at == 0, extra, below)
                above = jnp.where(y_at == EY - 1, extra, above)
            x_plus = 0.5 * (mine + visc[at + 1, rows])
            x_minus = 0.5 * (mine + visc[at - 1, rows])
            y_plus = 0.5 * (mine + above)
            y_minus = 0.5 * (mine + below)
            z_plus = 0.5 * (mine + visc[at, first + 1 : first + 1 + count])
            z_minus = 0.5 * (mine + visc[at, first - 1 : first - 1 + count])
            total = x_plus + x_minus + y_plus + y_minus + z_plus + z_minus
            inside = mine > 0.0
            inverse = jnp.where(inside, 1.0 / jnp.where(inside, total, 1.0), 0.0)
            inv[g, here] = inverse
            diag[g, here] = total
            for i, face in enumerate((x_minus, x_plus, y_minus, y_plus, z_minus, z_plus)):
                coef[i, g, here] = face * inverse
            for c in range(3):
                if first == 8:
                    value = low_z[c * SLABS + g]
                elif first == 144:
                    value = high_z[c * SLABS + g]
                else:
                    value = f[c, g, first - 16 : first - 16 + count]
                d0[c, at, rows] = value * inverse * (1.0 / MIDDLE)
        return 0

    lax.fori_loop(0, SLABS, setup, 0)
    ghosts(d0, range(3))

    def neighbours(ref, c, g, first, count):
        at = g + 1
        rows = slice(first, first + count)
        here = slice(first - 8, first - 8 + count)
        mine = ref[c, at, rows]
        below, above = pltpu.roll(mine, 1, 1), pltpu.roll(mine, LANES - 1, 1)
        x_minus, x_plus = ref[c, at - 1, rows], ref[c, at + 1, rows]
        z_minus = ref[c, at, first - 1 : first - 1 + count]
        z_plus = ref[c, at, first + 1 : first + 1 + count]
        total = coef[0, g, here] * x_minus + coef[1, g, here] * x_plus
        total = total + (coef[2, g, here] * below + coef[3, g, here] * above)
        total = total + (coef[4, g, here] * z_minus + coef[5, g, here] * z_plus)
        return mine, total, (x_minus, x_plus, below, above, z_minus, z_plus)

    def smooth():
        factors = chebyshev_factors()
        old = (d0, d1, d2)
        for step in range(CHEB - 1):
            scale_d, scale_r = factors[step]
            source = old[step]
            last = step == CHEB - 2

            def body(g, _):
                for first, count in PIECES:
                    rows = slice(first, first + count)
                    here = slice(first - 8, first - 8 + count)
                    for c in range(3):
                        mine, total, _ = neighbours(source, c, g, first, count)
                        if step == 0:
                            left = (MIDDLE - 1.0) * mine + total
                        else:
                            left = r[c, g, here] - mine + total
                        new = scale_d * mine + scale_r * left
                        if last:
                            s[c, g + 1, rows] = d0[c, g + 1, rows] + d1[c, g + 1, rows] + mine + new
                        else:
                            r[c, g, here] = left
                            old[step + 1][c, g + 1, rows] = new
                return 0

            lax.fori_loop(0, SLABS, body, 0)
            ghosts(s if last else old[step + 1], range(3))

    smooth()

    def apply_first(g, _):
        at = g + 1
        for first, count in PIECES:
            rows = slice(first, first + count)
            here = slice(first - 8, first - 8 + count)
            own = slice(first - 16, first - 16 + count)
            is_own = 16 <= first < 144
            flow = None
            for c in range(3):
                mine, total, sides = neighbours(s, c, g, first, count)
                value = diag[g, here] * (mine - total)
                slope = sides[2 * c + 1] - sides[2 * c]
                flow = slope if flow is None else flow + slope
                d0[c, at, rows] = value * inv[g, here] * (1.0 / MIDDLE)
                if is_own:
                    u1_out[c, g, own] = value
                    s0_out[c, g, own] = mine
            flow = -0.5 * flow
            p[at, rows] = visc[at, rows] * flow
            if is_own:
                u1_out[3, g, own] = flow
        return 0

    lax.fori_loop(0, SLABS, apply_first, 0)
    ghosts(d0, range(3))
    ghosts(p, [None])
    smooth()

    def apply_second(g, carry):
        at = g + 1
        lane = lane_index(8)
        y_at = lane & (EY - 1)
        x_at = (lane // EY) * SLABS + g
        own_cells = (x_at >= H) & (x_at < H + BX) & (y_at >= H) & (y_at < H + BY)
        acc = [jnp.zeros((8, LANES), jnp.float32) for _ in range(5)]
        for first, count in OWN_PIECES:
            rows = slice(first, first + count)
            here = slice(first - 8, first - 8 + count)
            own = slice(first - 16, first - 16 + count)
            centre = p[at, rows]
            press = (
                p[at - 1, rows],
                p[at + 1, rows],
                pltpu.roll(centre, 1, 1),
                pltpu.roll(centre, LANES - 1, 1),
                p[at, first - 1 : first - 1 + count],
                p[at, first + 1 : first + 1 + count],
            )
            flow = None
            values = []
            for c in range(3):
                mine, total, sides = neighbours(s, c, g, first, count)
                value = diag[g, here] * (mine - total) + 0.5 * (press[2 * c + 1] - press[2 * c])
                slope = sides[2 * c + 1] - sides[2 * c]
                flow = slope if flow is None else flow + slope
                s1_out[c, g, own] = mine
                values.append(value)
            values.append(-0.5 * flow)
            s1_out[3, g, own] = centre
            parts = [None] * 5
            for c in range(4):
                u2 = values[c]
                u2_out[c, g, own] = u2
                u1 = u1_out[c, g, own]
                pairs = [None, None, u1 * u1, u1 * u2, u2 * u2]
                if c < 3:
                    u0 = f[c, g, own]
                    pairs[0], pairs[1] = u0 * u1, u0 * u2
                for i, pair in enumerate(pairs):
                    if pair is not None:
                        parts[i] = pair if parts[i] is None else parts[i] + pair
            for i in range(5):
                acc[i] = acc[i] + (parts[i][:8] + parts[i][8:])
        return tuple(c + jnp.where(own_cells, a, 0.0) for c, a in zip(carry, acc))

    start = tuple(jnp.zeros((8, LANES), jnp.float32) for _ in range(5))
    acc = lax.fori_loop(0, SLABS, apply_second, start)
    lane = lane_index(1)
    line = jnp.zeros((1, LANES), jnp.float32)
    for i in range(5):
        both = jnp.sum(jnp.sum(acc[i], axis=0, keepdims=True), axis=1, keepdims=True)
        line = jnp.where(lane == i, both, line)
    sums[...] = line


def combine(gathered, f, s0, u1, s1, u2, solution_out, residual_out):
    line = jnp.sum(gathered[...], axis=0, keepdims=True)
    lane = lane_index(1)

    def entry(i):
        return jnp.sum(jnp.where(lane == i, line, 0.0), axis=1, keepdims=True)

    g01, g02, g11, g12, g22 = (entry(i) for i in range(5))
    lower = g12 / g11
    pivot = g22 - lower * g12
    b = (g02 - lower * g01) / pivot
    a = (g01 - g12 * b) / g11
    for g in range(SLABS):
        for c in range(4):
            if c < 3:
                sol = a * s0[c, g] + b * s1[c, g]
                res = f[c, g] - a * u1[c, g] - b * u2[c, g]
            else:
                sol = b * s1[c, g]
                res = -a * u1[c, g] - b * u2[c, g]
            for out, value in ((solution_out, sol), (residual_out, res)):
                back = value.T
                for k in range(CHUNKS):
                    x = k * SLABS + g - H
                    if 0 <= x < BX:
                        out[c, x] = back[k * EY + H : k * EY + H + BY]


def struct(*shape):
    return jax.ShapeDtypeStruct(shape, jnp.float32)


def call(kernel, outs, scratch=(), name=None):
    vmem = pl.BlockSpec(memory_space=pltpu.VMEM)

    def run(*args):
        return pl.pallas_call(
            kernel,
            out_shape=outs,
            in_specs=[vmem] * len(args),
            out_specs=[vmem] * len(outs),
            scratch_shapes=list(scratch),
            compiler_params=pltpu.CompilerParams(vmem_limit_bytes=60 * 1024 * 1024),
            name=name,
        )(*args)

    return run


def swap(tail, head, axis):
    count = lax.axis_size(axis)
    up = [(i, i + 1) for i in range(count - 1)]
    down = [(i + 1, i) for i in range(count - 1)]
    return lax.ppermute(tail, axis, up), lax.ppermute(head, axis, down)


def shards(viscosity, force):
    tail = jnp.concatenate([force[:, BX - 8 :].reshape(24, BY, BZ), viscosity[BX - 9 :]], axis=0)
    head = jnp.concatenate([force[:, :8].reshape(24, BY, BZ), viscosity[:9]], axis=0)
    low_x, high_x = swap(tail, head, "gx")
    tail, head = call(pack_y, [struct(YTILES, 8, BZ)] * 2, name="pack_y")(
        force, viscosity, low_x, high_x
    )
    low_y, high_y = swap(tail, head, "gy")
    field = (SLABS, BZ, LANES)
    f, v, ry, ex, tail, head = call(
        to_lanes,
        [struct(3, *field), struct(*field), struct(*field), struct(BZ, LANES)]
        + [struct(ZTILES, 8, LANES)] * 2,
        name="to_lanes",
    )(force, viscosity, low_x, high_x, low_y, high_y)
    low_z, high_z = swap(tail, head, "gz")
    ghosted = (SLABS + 2, ROWS, LANES)
    plain = (SLABS, EZ, LANES)
    shapes = [ghosted, (6, *plain), plain, plain] + [(3, *ghosted)] * 4 + [(3, *plain), ghosted]
    s0, u1, s1, u2, sums = call(
        solve_local,
        [struct(3, *field), struct(4, *field), struct(4, *field), struct(4, *field), struct(1, LANES)],
        [pltpu.VMEM(shape, jnp.float32) for shape in shapes],
        name="solve_local",
    )(f, v, ry, ex, low_z, high_z)
    devices = lax.axis_size(AXES)
    rows = jnp.broadcast_to(sums[None], (devices, 1, LANES))
    gathered = lax.all_to_all(rows, AXES, 0, 0).reshape(devices, LANES)
    block = struct(4, BX, BY, BZ)
    return tuple(call(combine, [block, block], name="combine")(gathered, f, s0, u1, s1, u2))


def solution(mesh):
    return jax.shard_map(
        shards,
        mesh=mesh,
        in_specs=(P("gx", "gy", "gz"), P(None, "gx", "gy", "gz")),
        out_specs=(P(None, "gx", "gy", "gz"), P(None, "gx", "gy", "gz")),
        check_vma=False,
    )
```

```python
import functools

import jax
import jax.numpy as jnp
from jax import lax
from jax.experimental import pallas as pl
from jax.experimental.pallas import tpu as pltpu
from jax.sharding import PartitionSpec as P

CHEB = 4
LOW_EDGE = 0.25
HIGH_EDGE = 2.0
MIDDLE = 0.5 * (HIGH_EDGE + LOW_EDGE)
HALF = 0.5 * (HIGH_EDGE - LOW_EDGE)
AXES = ("gx", "gy", "gz")

BX, BY, BZ, H = 32, 16, 128, 8
EX, EY, EZ = BX + 2 * H, BY + 2 * H, BZ + 2 * H
CHUNKS = 4
UNROLL = 2
SLABS = EX // CHUNKS
LANES = CHUNKS * EY
ROWS = EZ + 16
ZTILES = 4 * SLABS + 2
OWN = slice(16, 16 + BZ)
PIECES = [(8, 8)] + [(16 + 16 * i, 16) for i in range(8)] + [(144, 8)]
OWN_PIECES = PIECES[1:-1]


def smoother_polynomial():
    def minus_operator(p):
        return [high - low for low, high in zip(p + [0.0], [0.0] + p)]

    def plus(p, q):
        size = max(len(p), len(q))
        return [x + y for x, y in zip(p + [0.0] * (size - len(p)), q + [0.0] * (size - len(q)))]

    scaled = MIDDLE / HALF
    now = 1.0 / scaled
    update, remainder = [1.0 / MIDDLE], [1.0]
    result = update
    for _ in range(CHEB - 1):
        remainder = plus(remainder, minus_operator(update))
        following = 1.0 / (2.0 * scaled - now)
        update = plus(
            [following * now * x for x in update], [2.0 * following / HALF * x for x in remainder]
        )
        result = plus(result, update)
        now = following
    return result


def shared_tiles(reach):
    def at(side, far):
        return H - far if side == 0 else H + BX - 1 + far

    tiles = []
    for side in (0, 1):
        for far in range(1, H + 1):
            rows, other = reach - far, 2 * reach - 8 - far
            if rows == 8 or far < other:
                tiles.append((at(side, far), rows, None if rows == 8 else at(side, other)))
    half = reach - 4
    tiles.append((at(0, half), 4, at(1, half)))
    return tiles


FORCE_TILES = shared_tiles(8)
VISC_TILES = shared_tiles(9)
FORCE_COUNT = BX + len(FORCE_TILES)
VISC_COUNT = BX + len(VISC_TILES)
NINTH = 3 * FORCE_COUNT + VISC_COUNT
YTILES = NINTH + BX // 8


def tile_places(c):
    base = c * FORCE_COUNT
    places = {H + x: (base + x, None, False) for x in range(BX)}
    for i, (first, rows, second) in enumerate(FORCE_TILES if c < 3 else VISC_TILES):
        places[first] = (base + BX + i, rows, False)
        if second is not None:
            places[second] = (base + BX + i, rows, True)
    return places


def kept_if(condition, value):
    return jnp.where(condition, value, 0.0)


def at_start(axis):
    return lax.axis_index(axis) == 0


def at_end(axis):
    return lax.axis_index(axis) == lax.axis_size(axis) - 1


def pack_x(force, visc, force_out, visc_out, tail, head):
    force_out[...] = force[...]
    visc_out[...] = visc[...]
    for c in range(3):
        tail[c * 8 : c * 8 + 8] = force[c, BX - 8 :]
        head[c * 8 : c * 8 + 8] = force[c, :8]
    tail[24:] = visc[BX - 9 :]
    head[24:] = visc[:9]


def pack_y(force, visc, low_x, high_x, tail, head):
    row = lax.broadcasted_iota(jnp.int32, (8, BZ), 0)
    from_below, from_above = ~at_start("gx"), ~at_end("gx")
    for out, up in ((tail, True), (head, False)):
        first = BY - 8 if up else 0
        rows = slice(first, first + 8)

        def tile(c, at):
            if at < H:
                if c < 3:
                    return low_x[c * 8 + at, rows, :]
                return kept_if(from_below, low_x[25 + at, rows, :])
            at = at - H - BX
            return high_x[c * 8 + at, rows, :] if c < 3 else kept_if(from_above, high_x[24 + at, rows, :])

        for c in range(4):
            base = c * FORCE_COUNT
            out[base : base + BX] = force[c, :, rows, :] if c < 3 else visc[:, rows, :]
            for i, (one, count, two) in enumerate(FORCE_TILES if c < 3 else VISC_TILES):
                value = tile(c, one)
                if two is not None:
                    other = tile(c, two)
                    if up:
                        value = jnp.where(row >= 8 - count, value, pltpu.roll(other, 8 - count, 0))
                    else:
                        value = jnp.where(row < count, value, pltpu.roll(other, count, 0))
                out[base + BX + i] = value
        ninth = first - 1 if up else 8
        for x in range(BX):
            out[NINTH + x // 8, x % 8 : x % 8 + 1, :] = visc[x, ninth : ninth + 1, :]


def to_lanes(force, visc, low_x, high_x, low_y, high_y, f_out, v_out, ry_out, ex_out, tail, head):
    x_below, x_above = ~at_start("gx"), ~at_end("gx")
    y_below, y_above = ~at_start("gy"), ~at_end("gy")
    places = [tile_places(c) for c in range(4)]

    def rows_of(c, at):
        x = at - H
        if x < 0:
            middle = low_x[c * 8 + at] if c < 3 else kept_if(x_below, low_x[25 + at])
        elif x >= BX:
            middle = high_x[c * 8 + x - BX] if c < 3 else kept_if(x_above, high_x[24 + x - BX])
        else:
            middle = force[c, x] if c < 3 else visc[x]
        if at not in places[c]:
            return [jnp.zeros((8, BZ), jnp.float32), middle, jnp.zeros((8, BZ), jnp.float32)]
        where, count, second = places[c][at]
        lower, upper = low_y[where], high_y[where]
        if second:
            lower, upper = pltpu.roll(lower, count, 0), pltpu.roll(upper, 8 - count, 0)
        if c == 3:
            lower, upper = kept_if(y_below, lower), kept_if(y_above, upper)
        return [lower, middle, upper]

    for c in range(4):
        for g in range(SLABS):
            parts = []
            for k in range(CHUNKS):
                parts += rows_of(c, k * SLABS + g)
            block = jnp.concatenate(parts, axis=0).T
            if c < 3:
                f_out[c, g] = block
            else:
                v_out[g] = block
                tail[4 * SLABS + g // 8, g % 8 : g % 8 + 1, :] = block[BZ - 9 : BZ - 8]
                head[4 * SLABS + g // 8, g % 8 : g % 8 + 1, :] = block[8:9]
            tail[c * SLABS + g] = block[BZ - 8 :]
            head[c * SLABS + g] = block[:8]
    for out in (tail, head):
        out[ZTILES - 1, SLABS - 8 :, :] = jnp.zeros((16 - SLABS, LANES), jnp.float32)
    nothing = jnp.zeros((EY - 2, BZ), jnp.float32)
    for g in range(SLABS):
        parts = []
        for k in range(CHUNKS):
            x = k * SLABS + g - H
            if 0 <= x < BX:
                at = NINTH + x // 8
                lower = kept_if(y_below, low_y[at, x % 8 : x % 8 + 1, :])
                upper = kept_if(y_above, high_y[at, x % 8 : x % 8 + 1, :])
            else:
                lower = upper = jnp.zeros((1, BZ), jnp.float32)
            parts += [lower, nothing, upper]
        ry_out[g] = jnp.concatenate(parts, axis=0).T
    side = jnp.zeros((8, BZ), jnp.float32)
    between = jnp.zeros((2 * EY, BZ), jnp.float32)
    ex_out[...] = jnp.concatenate(
        [
            side, kept_if(x_below, low_x[24]), side, between,
            side, kept_if(x_above, high_x[32]), side,
        ],
        axis=0,
    ).T


def lane_index(rows):
    return lax.broadcasted_iota(jnp.int32, (rows, LANES), 1)


def solve_local(
    f, v, ry, ex, low_z, high_z,
    s0_out, u1_out, s1_out, u2_out, sums,
    visc, coef, inv, diag, d0, d1, d2, s, p,
):
    z_below, z_above = ~at_start("gz"), ~at_end("gz")
    *shape, leading = smoother_polynomial()
    shape = [x / leading for x in shape]

    def place(g, _):
        visc[g + 1, 0:8] = jnp.zeros((8, LANES), jnp.float32)
        visc[g + 1, 152:160] = jnp.zeros((8, LANES), jnp.float32)
        visc[g + 1, 8:16] = kept_if(z_below, low_z[3 * SLABS + g])
        visc[g + 1, OWN] = v[g]
        visc[g + 1, 144:152] = kept_if(z_above, high_z[3 * SLABS + g])
        return 0

    lax.fori_loop(0, SLABS, place, 0)
    for g in range(SLABS):
        ninth = (4 * SLABS + g // 8, slice(g % 8, g % 8 + 1))
        visc[g + 1, 7:8] = kept_if(z_below, low_z[ninth])
        visc[g + 1, 152:153] = kept_if(z_above, high_z[ninth])
    for first, count in PIECES:
        rows = slice(first, first + count)
        before = pltpu.roll(visc[SLABS, rows], EY, 1)
        after = pltpu.roll(visc[1, rows], LANES - EY, 1)
        if 16 <= first < 144:
            lane = lane_index(count)
            extra = ex[first - 16 : first - 16 + count]
            before = jnp.where(lane < EY, extra, before)
            after = jnp.where(lane >= LANES - EY, extra, after)
        visc[0, rows] = before
        visc[SLABS + 1, rows] = after

    def border(ref, which):
        zero = jnp.zeros((8, LANES), jnp.float32)
        for c in which:
            for g in range(SLABS):
                at = (c, g + 1) if c is not None else (g + 1,)
                ref[(*at, slice(0, 8))] = zero
                ref[(*at, slice(152, 160))] = zero

    for ref in (d0, d1, d2, s):
        border(ref, range(3))
    border(p, [None])

    def ghosts(ref, which):
        for c in which:
            for first, count in PIECES:
                rows = slice(first, first + count)
                pre = (c,) if c is not None else ()
                ref[(*pre, 0, rows)] = pltpu.roll(ref[(*pre, SLABS, rows)], EY, 1)
                ref[(*pre, SLABS + 1, rows)] = pltpu.roll(ref[(*pre, 1, rows)], LANES - EY, 1)

    def setup(g, _):
        at = g + 1
        for first, count in PIECES:
            rows = slice(first, first + count)
            here = slice(first - 8, first - 8 + count)
            lane = lane_index(count)
            y_at = lane & (EY - 1)
            mine = visc[at, rows]
            below, above = pltpu.roll(mine, 1, 1), pltpu.roll(mine, LANES - 1, 1)
            if 16 <= first < 144:
                extra = ry[g, first - 16 : first - 16 + count]
                below = jnp.where(y_at == 0, extra, below)
                above = jnp.where(y_at == EY - 1, extra, above)
            x_plus = 0.5 * (mine + visc[at + 1, rows])
            x_minus = 0.5 * (mine + visc[at - 1, rows])
            y_plus = 0.5 * (mine + above)
            y_minus = 0.5 * (mine + below)
            z_plus = 0.5 * (mine + visc[at, first + 1 : first + 1 + count])
            z_minus = 0.5 * (mine + visc[at, first - 1 : first - 1 + count])
            total = x_plus + x_minus + y_plus + y_minus + z_plus + z_minus
            inside = mine > 0.0
            inverse = jnp.where(inside, 1.0 / jnp.where(inside, total, 1.0), 0.0)
            inv[g, here] = inverse
            diag[g, here] = total
            for i, face in enumerate((x_minus, x_plus, y_minus, y_plus, z_minus, z_plus)):
                coef[i, g, here] = face * inverse
            for c in range(3):
                if first == 8:
                    value = low_z[c * SLABS + g]
                elif first == 144:
                    value = high_z[c * SLABS + g]
                else:
                    value = f[c, g, first - 16 : first - 16 + count]
                d0[c, at, rows] = value * inverse * leading
        return 0

    lax.fori_loop(0, SLABS, setup, 0, unroll=UNROLL)
    ghosts(d0, range(3))

    def neighbours(ref, c, g, first, count):
        at = g + 1
        rows = slice(first, first + count)
        here = slice(first - 8, first - 8 + count)
        mine = ref[c, at, rows]
        below, above = pltpu.roll(mine, 1, 1), pltpu.roll(mine, LANES - 1, 1)
        x_minus, x_plus = ref[c, at - 1, rows], ref[c, at + 1, rows]
        z_minus = ref[c, at, first - 1 : first - 1 + count]
        z_plus = ref[c, at, first + 1 : first + 1 + count]
        total = coef[0, g, here] * x_minus + coef[1, g, here] * x_plus
        total = total + (coef[2, g, here] * below + coef[3, g, here] * above)
        total = total + (coef[4, g, here] * z_minus + coef[5, g, here] * z_plus)
        return mine, total, (x_minus, x_plus, below, above, z_minus, z_plus)

    def smooth():
        chain = (d0, d1, d2, s)
        for step in range(CHEB - 1):
            source, target = chain[step], chain[step + 1]
            weight = shape[CHEB - 2 - step]

            def body(g, _):
                for first, count in PIECES:
                    rows = slice(first, first + count)
                    for c in range(3):
                        _, total, _ = neighbours(source, c, g, first, count)
                        target[c, g + 1, rows] = total + weight * d0[c, g + 1, rows]
                return 0

            lax.fori_loop(0, SLABS, body, 0, unroll=UNROLL)
            ghosts(target, range(3))

    smooth()

    def apply_first(g, _):
        at = g + 1
        for first, count in PIECES:
            rows = slice(first, first + count)
            here = slice(first - 8, first - 8 + count)
            own = slice(first - 16, first - 16 + count)
            is_own = 16 <= first < 144
            flow = None
            for c in range(3):
                mine, total, sides = neighbours(s, c, g, first, count)
                value = diag[g, here] * (mine - total)
                slope = sides[2 * c + 1] - sides[2 * c]
                flow = slope if flow is None else flow + slope
                d0[c, at, rows] = value * inv[g, here] * leading
                if is_own:
                    u1_out[c, g, own] = value
                    s0_out[c, g, own] = mine
            flow = -0.5 * flow
            p[at, rows] = visc[at, rows] * flow
            if is_own:
                u1_out[3, g, own] = flow
        return 0

    lax.fori_loop(0, SLABS, apply_first, 0, unroll=UNROLL)
    ghosts(d0, range(3))
    ghosts(p, [None])
    smooth()

    def apply_second(g, carry):
        at = g + 1
        lane = lane_index(8)
        y_at = lane & (EY - 1)
        x_at = (lane // EY) * SLABS + g
        own_cells = (x_at >= H) & (x_at < H + BX) & (y_at >= H) & (y_at < H + BY)
        acc = [jnp.zeros((8, LANES), jnp.float32) for _ in range(5)]
        for first, count in OWN_PIECES:
            rows = slice(first, first + count)
            here = slice(first - 8, first - 8 + count)
            own = slice(first - 16, first - 16 + count)
            centre = p[at, rows]
            press = (
                p[at - 1, rows],
                p[at + 1, rows],
                pltpu.roll(centre, 1, 1),
                pltpu.roll(centre, LANES - 1, 1),
                p[at, first - 1 : first - 1 + count],
                p[at, first + 1 : first + 1 + count],
            )
            flow = None
            values = []
            for c in range(3):
                mine, total, sides = neighbours(s, c, g, first, count)
                value = diag[g, here] * (mine - total) + 0.5 * (press[2 * c + 1] - press[2 * c])
                slope = sides[2 * c + 1] - sides[2 * c]
                flow = slope if flow is None else flow + slope
                s1_out[c, g, own] = mine
                values.append(value)
            values.append(-0.5 * flow)
            s1_out[3, g, own] = centre
            parts = [None] * 5
            for c in range(4):
                u2 = values[c]
                u2_out[c, g, own] = u2
                u1 = u1_out[c, g, own]
                pairs = [None, None, u1 * u1, u1 * u2, u2 * u2]
                if c < 3:
                    u0 = f[c, g, own]
                    pairs[0], pairs[1] = u0 * u1, u0 * u2
                for i, pair in enumerate(pairs):
                    if pair is not None:
                        parts[i] = pair if parts[i] is None else parts[i] + pair
            for i in range(5):
                acc[i] = acc[i] + (parts[i][:8] + parts[i][8:])
        return tuple(c + jnp.where(own_cells, a, 0.0) for c, a in zip(carry, acc))

    start = tuple(jnp.zeros((8, LANES), jnp.float32) for _ in range(5))
    acc = lax.fori_loop(0, SLABS, apply_second, start, unroll=UNROLL)
    lane = lane_index(1)
    line = jnp.zeros((1, LANES), jnp.float32)
    for i in range(5):
        both = jnp.sum(jnp.sum(acc[i], axis=0, keepdims=True), axis=1, keepdims=True)
        line = jnp.where(lane == i, both, line)
    sums[...] = line


def combine(gathered, f, s0, u1, s1, u2, solution_out, residual_out):
    line = jnp.sum(gathered[...], axis=0, keepdims=True)
    lane = lane_index(1)

    def entry(i):
        return jnp.sum(jnp.where(lane == i, line, 0.0), axis=1, keepdims=True)

    g01, g02, g11, g12, g22 = (entry(i) for i in range(5))
    lower = g12 / g11
    pivot = g22 - lower * g12
    b = (g02 - lower * g01) / pivot
    a = (g01 - g12 * b) / g11
    for g in range(SLABS):
        for c in range(4):
            if c < 3:
                sol = a * s0[c, g] + b * s1[c, g]
                res = f[c, g] - a * u1[c, g] - b * u2[c, g]
            else:
                sol = b * s1[c, g]
                res = -a * u1[c, g] - b * u2[c, g]
            for out, value in ((solution_out, sol), (residual_out, res)):
                back = value.T
                for k in range(CHUNKS):
                    x = k * SLABS + g - H
                    if 0 <= x < BX:
                        out[c, x] = back[k * EY + H : k * EY + H + BY]


def struct(*shape):
    return jax.ShapeDtypeStruct(shape, jnp.float32)


def kept(*shape):
    return pltpu.VMEM(shape, jnp.float32)


def call(kernel, outs, scratch=(), name=None, mib=16):
    vmem = pl.BlockSpec(memory_space=pltpu.VMEM)

    def run(*args):
        return pl.pallas_call(
            kernel,
            out_shape=outs,
            in_specs=[vmem] * len(args),
            out_specs=[vmem] * len(outs),
            scratch_shapes=list(scratch),
            compiler_params=pltpu.CompilerParams(vmem_limit_bytes=mib * 1024 * 1024),
            name=name,
        )(*args)

    return run


def swap(tail, head, axis):
    count = lax.axis_size(axis)
    up = [(i, (i + 1) % count) for i in range(count)]
    down = [(j, i) for i, j in up]
    return lax.ppermute(tail, axis, up), lax.ppermute(head, axis, down)


def shards(viscosity, force):
    force, viscosity, tail, head = call(
        pack_x,
        [kept(3, BX, BY, BZ), kept(BX, BY, BZ)] + [kept(33, BY, BZ)] * 2,
        name="pack_x",
    )(force, viscosity)
    low_x, high_x = swap(tail, head, "gx")
    tail, head = call(pack_y, [kept(YTILES, 8, BZ)] * 2, name="pack_y")(
        force, viscosity, low_x, high_x
    )
    low_y, high_y = swap(tail, head, "gy")
    field = (SLABS, BZ, LANES)
    f, v, ry, ex, tail, head = call(
        to_lanes,
        [kept(3, *field), kept(*field), kept(*field), kept(BZ, LANES)]
        + [kept(ZTILES, 8, LANES)] * 2,
        name="to_lanes",
    )(force, viscosity, low_x, high_x, low_y, high_y)
    low_z, high_z = swap(tail, head, "gz")
    ghosted = (SLABS + 2, ROWS, LANES)
    plain = (SLABS, EZ, LANES)
    shapes = [ghosted, (6, *plain), plain, plain] + [(3, *ghosted)] * 4 + [ghosted]
    s0, u1, s1, u2, sums = call(
        solve_local,
        [kept(3, *field), kept(4, *field), kept(4, *field), kept(4, *field), kept(1, LANES)],
        [pltpu.VMEM(shape, jnp.float32) for shape in shapes],
        name="solve_local",
        mib=32,
    )(f, v, ry, ex, low_z, high_z)
    devices = lax.axis_size(AXES)
    rows = jnp.broadcast_to(sums[None], (devices, 1, LANES))
    gathered = lax.all_to_all(rows, AXES, 0, 0).reshape(devices, LANES)
    block = struct(4, BX, BY, BZ)
    return tuple(call(combine, [block, block], name="combine")(gathered, f, s0, u1, s1, u2))


def solution(mesh):
    return jax.shard_map(
        shards,
        mesh=mesh,
        in_specs=(P("gx", "gy", "gz"), P(None, "gx", "gy", "gz")),
        out_specs=(P(None, "gx", "gy", "gz"), P(None, "gx", "gy", "gz")),
        check_vma=False,
    )
```

```python
import functools

import jax
import jax.numpy as jnp
from jax import lax
from jax.experimental import pallas as pl
from jax.experimental.pallas import tpu as pltpu
from jax.sharding import PartitionSpec as P

CHEB = 4
LOW_EDGE = 0.25
HIGH_EDGE = 2.0
MIDDLE = 0.5 * (HIGH_EDGE + LOW_EDGE)
HALF = 0.5 * (HIGH_EDGE - LOW_EDGE)
AXES = ("gx", "gy", "gz")

BX, BY, BZ, H = 32, 16, 128, 8
EX, EY, EZ = BX + 2 * H, BY + 2 * H, BZ + 2 * H
CHUNKS = 4
UNROLL = 4
SLABS = EX // CHUNKS
LANES = CHUNKS * EY
ROWS = EZ + 16
ZTILES = 4 * SLABS + 2
OWN = slice(16, 16 + BZ)
PIECES = [(8, 8)] + [(16 + 16 * i, 16) for i in range(8)] + [(144, 8)]
OWN_PIECES = PIECES[1:-1]


def smoother_polynomial():
    def minus_operator(p):
        return [high - low for low, high in zip(p + [0.0], [0.0] + p)]

    def plus(p, q):
        size = max(len(p), len(q))
        return [x + y for x, y in zip(p + [0.0] * (size - len(p)), q + [0.0] * (size - len(q)))]

    scaled = MIDDLE / HALF
    now = 1.0 / scaled
    update, remainder = [1.0 / MIDDLE], [1.0]
    result = update
    for _ in range(CHEB - 1):
        remainder = plus(remainder, minus_operator(update))
        following = 1.0 / (2.0 * scaled - now)
        update = plus(
            [following * now * x for x in update], [2.0 * following / HALF * x for x in remainder]
        )
        result = plus(result, update)
        now = following
    return result


def shared_tiles(reach):
    def at(side, far):
        return H - far if side == 0 else H + BX - 1 + far

    tiles = []
    for side in (0, 1):
        for far in range(1, H + 1):
            rows, other = reach - far, 2 * reach - 8 - far
            if rows == 8 or far < other:
                tiles.append((at(side, far), rows, None if rows == 8 else at(side, other)))
    half = reach - 4
    tiles.append((at(0, half), 4, at(1, half)))
    return tiles


FORCE_TILES = shared_tiles(8)
VISC_TILES = shared_tiles(9)
FACE_TILES = 4 * BX + BX // 8
CORNER_TILES = 3 * len(FORCE_TILES) + len(VISC_TILES)


def corner_places(c):
    places = {}
    for i, (first, rows, second) in enumerate(FORCE_TILES if c < 3 else VISC_TILES):
        at = c * len(FORCE_TILES) + i
        places[first] = (at, rows, False)
        if second is not None:
            places[second] = (at, rows, True)
    return places


def kept_if(condition, value):
    return jnp.where(condition, value, 0.0)


def at_start(axis):
    return lax.axis_index(axis) == 0


def at_end(axis):
    return lax.axis_index(axis) == lax.axis_size(axis) - 1


def pack_faces(force_in, visc_in, force, visc, tail_x, head_x, tail_y, head_y, arrived):
    copies = [
        pltpu.make_async_copy(visc_in, visc, arrived.at[0]),
        pltpu.make_async_copy(force_in, force, arrived.at[1]),
    ]
    for copy in copies:
        copy.start()
    copies[0].wait()
    tail_x[24:] = visc[BX - 9 :]
    head_x[24:] = visc[:9]
    for out, first, ninth in ((tail_y, BY - 8, BY - 9), (head_y, 0, 8)):
        out[3 * BX : 4 * BX] = visc[:, first : first + 8, :]
        for x in range(BX):
            out[4 * BX + x // 8, x % 8 : x % 8 + 1, :] = visc[x, ninth : ninth + 1, :]
    copies[1].wait()
    for c in range(3):
        tail_x[c * 8 : c * 8 + 8] = force[c, BX - 8 :]
        head_x[c * 8 : c * 8 + 8] = force[c, :8]
        tail_y[c * BX : c * BX + BX] = force[c, :, BY - 8 :, :]
        head_y[c * BX : c * BX + BX] = force[c, :, :8, :]


def pack_corners(low_x, high_x, tail, head):
    row = lax.broadcasted_iota(jnp.int32, (8, BZ), 0)
    from_below, from_above = ~at_start("gx"), ~at_end("gx")
    for out, up in ((tail, True), (head, False)):
        first = BY - 8 if up else 0
        rows = slice(first, first + 8)

        def tile(c, at):
            if at < H:
                if c < 3:
                    return low_x[c * 8 + at, rows, :]
                return kept_if(from_below, low_x[25 + at, rows, :])
            at = at - H - BX
            return high_x[c * 8 + at, rows, :] if c < 3 else kept_if(from_above, high_x[24 + at, rows, :])

        for c in range(4):
            for i, (one, count, two) in enumerate(FORCE_TILES if c < 3 else VISC_TILES):
                value = tile(c, one)
                if two is not None:
                    other = tile(c, two)
                    if up:
                        value = jnp.where(row >= 8 - count, value, pltpu.roll(other, 8 - count, 0))
                    else:
                        value = jnp.where(row < count, value, pltpu.roll(other, count, 0))
                out[c * len(FORCE_TILES) + i] = value


def to_lanes(
    force, visc, low_x, high_x, low_y, high_y, low_c, high_c,
    f_out, v_out, ry_out, ex_out, tail, head,
):
    x_below, x_above = ~at_start("gx"), ~at_end("gx")
    y_below, y_above = ~at_start("gy"), ~at_end("gy")
    places = [corner_places(c) for c in range(4)]

    def rows_of(c, at):
        x = at - H
        if x < 0:
            middle = low_x[c * 8 + at] if c < 3 else kept_if(x_below, low_x[25 + at])
        elif x >= BX:
            middle = high_x[c * 8 + x - BX] if c < 3 else kept_if(x_above, high_x[24 + x - BX])
        else:
            middle = force[c, x] if c < 3 else visc[x]
        if 0 <= x < BX:
            lower, upper = low_y[c * BX + x], high_y[c * BX + x]
        elif at in places[c]:
            where, count, second = places[c][at]
            lower, upper = low_c[where], high_c[where]
            if second:
                lower, upper = pltpu.roll(lower, count, 0), pltpu.roll(upper, 8 - count, 0)
        else:
            lower = upper = jnp.zeros((8, BZ), jnp.float32)
        if c == 3:
            lower, upper = kept_if(y_below, lower), kept_if(y_above, upper)
        return [lower, middle, upper]

    for c in range(4):
        for g in range(SLABS):
            parts = []
            for k in range(CHUNKS):
                parts += rows_of(c, k * SLABS + g)
            block = jnp.concatenate(parts, axis=0).T
            if c < 3:
                f_out[c, g] = block
            else:
                v_out[g] = block
                tail[4 * SLABS + g // 8, g % 8 : g % 8 + 1, :] = block[BZ - 9 : BZ - 8]
                head[4 * SLABS + g // 8, g % 8 : g % 8 + 1, :] = block[8:9]
            tail[c * SLABS + g] = block[BZ - 8 :]
            head[c * SLABS + g] = block[:8]
    for out in (tail, head):
        out[ZTILES - 1, SLABS - 8 :, :] = jnp.zeros((16 - SLABS, LANES), jnp.float32)
    nothing = jnp.zeros((EY - 2, BZ), jnp.float32)
    for g in range(SLABS):
        parts = []
        for k in range(CHUNKS):
            x = k * SLABS + g - H
            if 0 <= x < BX:
                at = 4 * BX + x // 8
                lower = kept_if(y_below, low_y[at, x % 8 : x % 8 + 1, :])
                upper = kept_if(y_above, high_y[at, x % 8 : x % 8 + 1, :])
            else:
                lower = upper = jnp.zeros((1, BZ), jnp.float32)
            parts += [lower, nothing, upper]
        ry_out[g] = jnp.concatenate(parts, axis=0).T
    side = jnp.zeros((8, BZ), jnp.float32)
    between = jnp.zeros((2 * EY, BZ), jnp.float32)
    ex_out[...] = jnp.concatenate(
        [
            side, kept_if(x_below, low_x[24]), side, between,
            side, kept_if(x_above, high_x[32]), side,
        ],
        axis=0,
    ).T


def lane_index(rows):
    return lax.broadcasted_iota(jnp.int32, (rows, LANES), 1)


def solve_local(
    f, v, ry, ex, low_z, high_z,
    s0_out, u1_out, s1_out, u2_out, sums,
    visc, coef, inv, diag, d0, d1, d2, s, p,
):
    z_below, z_above = ~at_start("gz"), ~at_end("gz")
    *shape, leading = smoother_polynomial()
    shape = [x / leading for x in shape]

    def place(g, _):
        visc[g + 1, 0:8] = jnp.zeros((8, LANES), jnp.float32)
        visc[g + 1, 152:160] = jnp.zeros((8, LANES), jnp.float32)
        visc[g + 1, 8:16] = kept_if(z_below, low_z[3 * SLABS + g])
        visc[g + 1, OWN] = v[g]
        visc[g + 1, 144:152] = kept_if(z_above, high_z[3 * SLABS + g])
        return 0

    lax.fori_loop(0, SLABS, place, 0)
    for g in range(SLABS):
        ninth = (4 * SLABS + g // 8, slice(g % 8, g % 8 + 1))
        visc[g + 1, 7:8] = kept_if(z_below, low_z[ninth])
        visc[g + 1, 152:153] = kept_if(z_above, high_z[ninth])
    for first, count in PIECES:
        rows = slice(first, first + count)
        before = pltpu.roll(visc[SLABS, rows], EY, 1)
        after = pltpu.roll(visc[1, rows], LANES - EY, 1)
        if 16 <= first < 144:
            lane = lane_index(count)
            extra = ex[first - 16 : first - 16 + count]
            before = jnp.where(lane < EY, extra, before)
            after = jnp.where(lane >= LANES - EY, extra, after)
        visc[0, rows] = before
        visc[SLABS + 1, rows] = after

    def border(ref, which):
        zero = jnp.zeros((8, LANES), jnp.float32)
        for c in which:
            for g in range(SLABS):
                at = (c, g + 1) if c is not None else (g + 1,)
                ref[(*at, slice(0, 8))] = zero
                ref[(*at, slice(152, 160))] = zero

    for ref in (d0, d1, d2, s):
        border(ref, range(3))
    border(p, [None])

    def ghosts(ref, which):
        for c in which:
            for first, count in PIECES:
                rows = slice(first, first + count)
                pre = (c,) if c is not None else ()
                ref[(*pre, 0, rows)] = pltpu.roll(ref[(*pre, SLABS, rows)], EY, 1)
                ref[(*pre, SLABS + 1, rows)] = pltpu.roll(ref[(*pre, 1, rows)], LANES - EY, 1)

    def setup(g, _):
        at = g + 1
        for first, count in PIECES:
            rows = slice(first, first + count)
            here = slice(first - 8, first - 8 + count)
            lane = lane_index(count)
            y_at = lane & (EY - 1)
            mine = visc[at, rows]
            below, above = pltpu.roll(mine, 1, 1), pltpu.roll(mine, LANES - 1, 1)
            if 16 <= first < 144:
                extra = ry[g, first - 16 : first - 16 + count]
                below = jnp.where(y_at == 0, extra, below)
                above = jnp.where(y_at == EY - 1, extra, above)
            x_plus = 0.5 * (mine + visc[at + 1, rows])
            x_minus = 0.5 * (mine + visc[at - 1, rows])
            y_plus = 0.5 * (mine + above)
            y_minus = 0.5 * (mine + below)
            z_plus = 0.5 * (mine + visc[at, first + 1 : first + 1 + count])
            z_minus = 0.5 * (mine + visc[at, first - 1 : first - 1 + count])
            total = x_plus + x_minus + y_plus + y_minus + z_plus + z_minus
            inside = mine > 0.0
            inverse = jnp.where(inside, 1.0 / jnp.where(inside, total, 1.0), 0.0)
            inv[g, here] = inverse
            diag[g, here] = total
            for i, face in enumerate((x_minus, x_plus, y_minus, y_plus, z_minus, z_plus)):
                coef[i, g, here] = face * inverse
            for c in range(3):
                if first == 8:
                    value = low_z[c * SLABS + g]
                elif first == 144:
                    value = high_z[c * SLABS + g]
                else:
                    value = f[c, g, first - 16 : first - 16 + count]
                d0[c, at, rows] = value * inverse * leading
        return 0

    lax.fori_loop(0, SLABS, setup, 0, unroll=UNROLL)
    ghosts(d0, range(3))

    def neighbours(ref, c, g, first, count):
        at = g + 1
        rows = slice(first, first + count)
        here = slice(first - 8, first - 8 + count)
        mine = ref[c, at, rows]
        below, above = pltpu.roll(mine, 1, 1), pltpu.roll(mine, LANES - 1, 1)
        x_minus, x_plus = ref[c, at - 1, rows], ref[c, at + 1, rows]
        z_minus = ref[c, at, first - 1 : first - 1 + count]
        z_plus = ref[c, at, first + 1 : first + 1 + count]
        total = coef[0, g, here] * x_minus + coef[1, g, here] * x_plus
        total = total + (coef[2, g, here] * below + coef[3, g, here] * above)
        total = total + (coef[4, g, here] * z_minus + coef[5, g, here] * z_plus)
        return mine, total, (x_minus, x_plus, below, above, z_minus, z_plus)

    def smooth():
        chain = (d0, d1, d2, s)
        for step in range(CHEB - 1):
            source, target = chain[step], chain[step + 1]
            weight = shape[CHEB - 2 - step]

            def body(g, _):
                for first, count in PIECES:
                    rows = slice(first, first + count)
                    for c in range(3):
                        _, total, _ = neighbours(source, c, g, first, count)
                        target[c, g + 1, rows] = total + weight * d0[c, g + 1, rows]
                return 0

            lax.fori_loop(0, SLABS, body, 0, unroll=UNROLL)
            ghosts(target, range(3))

    smooth()

    def apply_first(g, _):
        at = g + 1
        for first, count in PIECES:
            rows = slice(first, first + count)
            here = slice(first - 8, first - 8 + count)
            own = slice(first - 16, first - 16 + count)
            is_own = 16 <= first < 144
            flow = None
            for c in range(3):
                mine, total, sides = neighbours(s, c, g, first, count)
                value = diag[g, here] * (mine - total)
                slope = sides[2 * c + 1] - sides[2 * c]
                flow = slope if flow is None else flow + slope
                d0[c, at, rows] = value * inv[g, here] * leading
                if is_own:
                    u1_out[c, g, own] = value
                    s0_out[c, g, own] = mine
            flow = -0.5 * flow
            p[at, rows] = visc[at, rows] * flow
            if is_own:
                u1_out[3, g, own] = flow
        return 0

    lax.fori_loop(0, SLABS, apply_first, 0, unroll=UNROLL)
    ghosts(d0, range(3))
    ghosts(p, [None])
    smooth()

    def apply_second(g, carry):
        at = g + 1
        lane = lane_index(8)
        y_at = lane & (EY - 1)
        x_at = (lane // EY) * SLABS + g
        own_cells = (x_at >= H) & (x_at < H + BX) & (y_at >= H) & (y_at < H + BY)
        acc = [jnp.zeros((8, LANES), jnp.float32) for _ in range(5)]
        for first, count in OWN_PIECES:
            rows = slice(first, first + count)
            here = slice(first - 8, first - 8 + count)
            own = slice(first - 16, first - 16 + count)
            centre = p[at, rows]
            press = (
                p[at - 1, rows],
                p[at + 1, rows],
                pltpu.roll(centre, 1, 1),
                pltpu.roll(centre, LANES - 1, 1),
                p[at, first - 1 : first - 1 + count],
                p[at, first + 1 : first + 1 + count],
            )
            flow = None
            values = []
            for c in range(3):
                mine, total, sides = neighbours(s, c, g, first, count)
                value = diag[g, here] * (mine - total) + 0.5 * (press[2 * c + 1] - press[2 * c])
                slope = sides[2 * c + 1] - sides[2 * c]
                flow = slope if flow is None else flow + slope
                s1_out[c, g, own] = mine
                values.append(value)
            values.append(-0.5 * flow)
            s1_out[3, g, own] = centre
            parts = [None] * 5
            for c in range(4):
                u2 = values[c]
                u2_out[c, g, own] = u2
                u1 = u1_out[c, g, own]
                pairs = [None, None, u1 * u1, u1 * u2, u2 * u2]
                if c < 3:
                    u0 = f[c, g, own]
                    pairs[0], pairs[1] = u0 * u1, u0 * u2
                for i, pair in enumerate(pairs):
                    if pair is not None:
                        parts[i] = pair if parts[i] is None else parts[i] + pair
            for i in range(5):
                acc[i] = acc[i] + (parts[i][:8] + parts[i][8:])
        return tuple(c + jnp.where(own_cells, a, 0.0) for c, a in zip(carry, acc))

    start = tuple(jnp.zeros((8, LANES), jnp.float32) for _ in range(5))
    acc = lax.fori_loop(0, SLABS, apply_second, start, unroll=UNROLL)
    lane = lane_index(1)
    line = jnp.zeros((1, LANES), jnp.float32)
    for i in range(5):
        both = jnp.sum(jnp.sum(acc[i], axis=0, keepdims=True), axis=1, keepdims=True)
        line = jnp.where(lane == i, both, line)
    sums[...] = line


def combine(gathered, f, s0, u1, s1, u2, solution_out, residual_out):
    line = jnp.sum(gathered[...], axis=0, keepdims=True)
    lane = lane_index(1)

    def entry(i):
        return jnp.sum(jnp.where(lane == i, line, 0.0), axis=1, keepdims=True)

    g01, g02, g11, g12, g22 = (entry(i) for i in range(5))
    lower = g12 / g11
    pivot = g22 - lower * g12
    b = (g02 - lower * g01) / pivot
    a = (g01 - g12 * b) / g11
    for g in range(SLABS):
        for c in range(4):
            if c < 3:
                sol = a * s0[c, g] + b * s1[c, g]
                res = f[c, g] - a * u1[c, g] - b * u2[c, g]
            else:
                sol = b * s1[c, g]
                res = -a * u1[c, g] - b * u2[c, g]
            for out, value in ((solution_out, sol), (residual_out, res)):
                back = value.T
                for k in range(CHUNKS):
                    x = k * SLABS + g - H
                    if 0 <= x < BX:
                        out[c, x] = back[k * EY + H : k * EY + H + BY]


def struct(*shape):
    return jax.ShapeDtypeStruct(shape, jnp.float32)


def kept(*shape):
    return pltpu.VMEM(shape, jnp.float32)


def call(kernel, outs, scratch=(), name=None, mib=16, source=pltpu.VMEM):
    vmem = pl.BlockSpec(memory_space=pltpu.VMEM)
    given = pl.BlockSpec(memory_space=source)

    def run(*args):
        return pl.pallas_call(
            kernel,
            out_shape=outs,
            in_specs=[given] * len(args),
            out_specs=[vmem] * len(outs),
            scratch_shapes=list(scratch),
            compiler_params=pltpu.CompilerParams(vmem_limit_bytes=mib * 1024 * 1024),
            name=name,
        )(*args)

    return run


def swap(tail, head, axis):
    count = lax.axis_size(axis)
    up = [(i, (i + 1) % count) for i in range(count)]
    down = [(j, i) for i, j in up]
    return lax.ppermute(tail, axis, up), lax.ppermute(head, axis, down)


def shards(viscosity, force):
    force, viscosity, tail_x, head_x, tail_y, head_y = call(
        pack_faces,
        [kept(3, BX, BY, BZ), kept(BX, BY, BZ)]
        + [kept(33, BY, BZ)] * 2
        + [kept(FACE_TILES, 8, BZ)] * 2,
        [pltpu.SemaphoreType.DMA((2,))],
        name="pack_faces",
        source=pltpu.HBM,
    )(*(pltpu.with_memory_space_constraint(x, pltpu.HBM) for x in (force, viscosity)))
    low_y, high_y = swap(tail_y, head_y, "gy")
    low_x, high_x = swap(tail_x, head_x, "gx")
    tail, head = call(pack_corners, [kept(CORNER_TILES, 8, BZ)] * 2, name="pack_corners")(
        low_x, high_x
    )
    low_c, high_c = swap(tail, head, "gy")
    field = (SLABS, BZ, LANES)
    f, v, ry, ex, tail, head = call(
        to_lanes,
        [kept(3, *field), kept(*field), kept(*field), kept(BZ, LANES)]
        + [kept(ZTILES, 8, LANES)] * 2,
        name="to_lanes",
    )(force, viscosity, low_x, high_x, low_y, high_y, low_c, high_c)
    low_z, high_z = swap(tail, head, "gz")
    ghosted = (SLABS + 2, ROWS, LANES)
    plain = (SLABS, EZ, LANES)
    shapes = [ghosted, (6, *plain), plain, plain] + [(3, *ghosted)] * 4 + [ghosted]
    s0, u1, s1, u2, sums = call(
        solve_local,
        [kept(3, *field), kept(4, *field), kept(4, *field), kept(4, *field), kept(1, LANES)],
        [pltpu.VMEM(shape, jnp.float32) for shape in shapes],
        name="solve_local",
        mib=32,
    )(f, v, ry, ex, low_z, high_z)
    devices = lax.axis_size(AXES)
    rows = jnp.broadcast_to(sums[None], (devices, 1, LANES))
    gathered = lax.all_to_all(rows, AXES, 0, 0).reshape(devices, LANES)
    block = struct(4, BX, BY, BZ)
    return tuple(call(combine, [block, block], name="combine")(gathered, f, s0, u1, s1, u2))


def solution(mesh):
    return jax.shard_map(
        shards,
        mesh=mesh,
        in_specs=(P("gx", "gy", "gz"), P(None, "gx", "gy", "gz")),
        out_specs=(P(None, "gx", "gy", "gz"), P(None, "gx", "gy", "gz")),
        check_vma=False,
    )
```

```python
import functools

import jax
import jax.numpy as jnp
from jax import lax
from jax.experimental import pallas as pl
from jax.experimental.pallas import tpu as pltpu
from jax.sharding import PartitionSpec as P

CHEB = 4
LOW_EDGE = 0.25
HIGH_EDGE = 2.0
MIDDLE = 0.5 * (HIGH_EDGE + LOW_EDGE)
HALF = 0.5 * (HIGH_EDGE - LOW_EDGE)
AXES = ("gx", "gy", "gz")

BX, BY, BZ, H = 32, 16, 128, 8
EX, EY, EZ = BX + 2 * H, BY + 2 * H, BZ + 2 * H
CHUNKS = 4
UNROLL = 12
SLABS = EX // CHUNKS
LANES = CHUNKS * EY
ROWS = EZ + 16
ZTILES = 4 * SLABS + 2
OWN = slice(16, 16 + BZ)
PIECES = [(8, 8)] + [(16 + 16 * i, 16) for i in range(8)] + [(144, 8)]
OWN_PIECES = PIECES[1:-1]
END_PIECES = [(8, 8), (16, 8), (136, 8), (144, 8)]


def smoother_polynomial():
    def minus_operator(p):
        return [high - low for low, high in zip(p + [0.0], [0.0] + p)]

    def plus(p, q):
        size = max(len(p), len(q))
        return [x + y for x, y in zip(p + [0.0] * (size - len(p)), q + [0.0] * (size - len(q)))]

    scaled = MIDDLE / HALF
    now = 1.0 / scaled
    update, remainder = [1.0 / MIDDLE], [1.0]
    result = update
    for _ in range(CHEB - 1):
        remainder = plus(remainder, minus_operator(update))
        following = 1.0 / (2.0 * scaled - now)
        update = plus(
            [following * now * x for x in update], [2.0 * following / HALF * x for x in remainder]
        )
        result = plus(result, update)
        now = following
    return result


def shared_tiles(reach):
    def at(side, far):
        return H - far if side == 0 else H + BX - 1 + far

    tiles = []
    for side in (0, 1):
        for far in range(1, H + 1):
            rows, other = reach - far, 2 * reach - 8 - far
            if rows == 8 or far < other:
                tiles.append((at(side, far), rows, None if rows == 8 else at(side, other)))
    half = reach - 4
    tiles.append((at(0, half), 4, at(1, half)))
    return tiles


FORCE_TILES = shared_tiles(8)
VISC_TILES = shared_tiles(9)
FACE_TILES = 4 * BX + BX // 8
CORNER_TILES = 3 * len(FORCE_TILES) + len(VISC_TILES)


def corner_places(c):
    places = {}
    for i, (first, rows, second) in enumerate(FORCE_TILES if c < 3 else VISC_TILES):
        at = c * len(FORCE_TILES) + i
        places[first] = (at, rows, False)
        if second is not None:
            places[second] = (at, rows, True)
    return places


def kept_if(condition, value):
    return jnp.where(condition, value, 0.0)


def at_start(axis):
    return lax.axis_index(axis) == 0


def at_end(axis):
    return lax.axis_index(axis) == lax.axis_size(axis) - 1


def pack_faces(force_in, visc_in, force, visc, tail_x, head_x, tail_y, head_y, arrived):
    copies = [
        pltpu.make_async_copy(visc_in, visc, arrived.at[0]),
        pltpu.make_async_copy(force_in, force, arrived.at[1]),
    ]
    for copy in copies:
        copy.start()
    copies[0].wait()
    tail_x[24:] = visc[BX - 9 :]
    head_x[24:] = visc[:9]
    for out, first, ninth in ((tail_y, BY - 8, BY - 9), (head_y, 0, 8)):
        out[3 * BX : 4 * BX] = visc[:, first : first + 8, :]
        for x in range(BX):
            out[4 * BX + x // 8, x % 8 : x % 8 + 1, :] = visc[x, ninth : ninth + 1, :]
    copies[1].wait()
    for c in range(3):
        tail_x[c * 8 : c * 8 + 8] = force[c, BX - 8 :]
        head_x[c * 8 : c * 8 + 8] = force[c, :8]
        tail_y[c * BX : c * BX + BX] = force[c, :, BY - 8 :, :]
        head_y[c * BX : c * BX + BX] = force[c, :, :8, :]


def pack_corners(low_x, high_x, tail, head):
    row = lax.broadcasted_iota(jnp.int32, (8, BZ), 0)
    from_below, from_above = ~at_start("gx"), ~at_end("gx")
    for out, up in ((tail, True), (head, False)):
        first = BY - 8 if up else 0
        rows = slice(first, first + 8)

        def tile(c, at):
            if at < H:
                if c < 3:
                    return low_x[c * 8 + at, rows, :]
                return kept_if(from_below, low_x[25 + at, rows, :])
            at = at - H - BX
            return high_x[c * 8 + at, rows, :] if c < 3 else kept_if(from_above, high_x[24 + at, rows, :])

        for c in range(4):
            for i, (one, count, two) in enumerate(FORCE_TILES if c < 3 else VISC_TILES):
                value = tile(c, one)
                if two is not None:
                    other = tile(c, two)
                    if up:
                        value = jnp.where(row >= 8 - count, value, pltpu.roll(other, 8 - count, 0))
                    else:
                        value = jnp.where(row < count, value, pltpu.roll(other, count, 0))
                out[c * len(FORCE_TILES) + i] = value


def to_lanes(
    force, visc, low_x, high_x, low_y, high_y, low_c, high_c,
    f_out, v_out, ry_out, ex_out, tail, head,
):
    x_below, x_above = ~at_start("gx"), ~at_end("gx")
    y_below, y_above = ~at_start("gy"), ~at_end("gy")
    places = [corner_places(c) for c in range(4)]

    def rows_of(c, at):
        x = at - H
        if x < 0:
            middle = low_x[c * 8 + at] if c < 3 else kept_if(x_below, low_x[25 + at])
        elif x >= BX:
            middle = high_x[c * 8 + x - BX] if c < 3 else kept_if(x_above, high_x[24 + x - BX])
        else:
            middle = force[c, x] if c < 3 else visc[x]
        if 0 <= x < BX:
            lower, upper = low_y[c * BX + x], high_y[c * BX + x]
        elif at in places[c]:
            where, count, second = places[c][at]
            lower, upper = low_c[where], high_c[where]
            if second:
                lower, upper = pltpu.roll(lower, count, 0), pltpu.roll(upper, 8 - count, 0)
        else:
            lower = upper = jnp.zeros((8, BZ), jnp.float32)
        if c == 3:
            lower, upper = kept_if(y_below, lower), kept_if(y_above, upper)
        return [lower, middle, upper]

    for c in range(4):
        for g in range(SLABS):
            parts = []
            for k in range(CHUNKS):
                parts += rows_of(c, k * SLABS + g)
            block = jnp.concatenate(parts, axis=0).T
            if c < 3:
                f_out[c, g] = block
            else:
                v_out[g] = block
                tail[4 * SLABS + g // 8, g % 8 : g % 8 + 1, :] = block[BZ - 9 : BZ - 8]
                head[4 * SLABS + g // 8, g % 8 : g % 8 + 1, :] = block[8:9]
            tail[c * SLABS + g] = block[BZ - 8 :]
            head[c * SLABS + g] = block[:8]
    for out in (tail, head):
        out[ZTILES - 1, SLABS - 8 :, :] = jnp.zeros((16 - SLABS, LANES), jnp.float32)
    nothing = jnp.zeros((EY - 2, BZ), jnp.float32)
    for g in range(SLABS):
        parts = []
        for k in range(CHUNKS):
            x = k * SLABS + g - H
            if 0 <= x < BX:
                at = 4 * BX + x // 8
                lower = kept_if(y_below, low_y[at, x % 8 : x % 8 + 1, :])
                upper = kept_if(y_above, high_y[at, x % 8 : x % 8 + 1, :])
            else:
                lower = upper = jnp.zeros((1, BZ), jnp.float32)
            parts += [lower, nothing, upper]
        ry_out[g] = jnp.concatenate(parts, axis=0).T
    side = jnp.zeros((8, BZ), jnp.float32)
    between = jnp.zeros((2 * EY, BZ), jnp.float32)
    ex_out[...] = jnp.concatenate(
        [
            side, kept_if(x_below, low_x[24]), side, between,
            side, kept_if(x_above, high_x[32]), side,
        ],
        axis=0,
    ).T


def lane_index(rows):
    return lax.broadcasted_iota(jnp.int32, (rows, LANES), 1)


def ghosts(ref, which, pieces):
    for c in which:
        for first, count in pieces:
            rows = slice(first, first + count)
            pre = (c,) if c is not None else ()
            ref[(*pre, 0, rows)] = pltpu.roll(ref[(*pre, SLABS, rows)], EY, 1)
            ref[(*pre, SLABS + 1, rows)] = pltpu.roll(ref[(*pre, 1, rows)], LANES - EY, 1)


def set_up(f, ry, visc, coef, inv, diag, d0, halo, leading, pieces):
    def body(g, _):
        at = g + 1
        for first, count in pieces:
            rows = slice(first, first + count)
            here = slice(first - 8, first - 8 + count)
            lane = lane_index(count)
            y_at = lane & (EY - 1)
            mine = visc[at, rows]
            below, above = pltpu.roll(mine, 1, 1), pltpu.roll(mine, LANES - 1, 1)
            if 16 <= first < 144:
                extra = ry[g, first - 16 : first - 16 + count]
                below = jnp.where(y_at == 0, extra, below)
                above = jnp.where(y_at == EY - 1, extra, above)
            x_plus = 0.5 * (mine + visc[at + 1, rows])
            x_minus = 0.5 * (mine + visc[at - 1, rows])
            y_plus = 0.5 * (mine + above)
            y_minus = 0.5 * (mine + below)
            z_plus = 0.5 * (mine + visc[at, first + 1 : first + 1 + count])
            z_minus = 0.5 * (mine + visc[at, first - 1 : first - 1 + count])
            total = x_plus + x_minus + y_plus + y_minus + z_plus + z_minus
            inside = mine > 0.0
            inverse = jnp.where(inside, 1.0 / jnp.where(inside, total, 1.0), 0.0)
            inv[g, here] = inverse
            diag[g, here] = total
            for i, face in enumerate((x_minus, x_plus, y_minus, y_plus, z_minus, z_plus)):
                coef[i, g, here] = face * inverse
            for c in range(3):
                if first == 8:
                    value = halo[0][c * SLABS + g]
                elif first == 144:
                    value = halo[1][c * SLABS + g]
                else:
                    value = f[c, g, first - 16 : first - 16 + count]
                d0[c, at, rows] = value * inverse * leading
        return 0

    lax.fori_loop(0, SLABS, body, 0, unroll=UNROLL)
    ghosts(d0, range(3), pieces)


def neighbours(coef, ref, c, g, first, count):
    at = g + 1
    rows = slice(first, first + count)
    here = slice(first - 8, first - 8 + count)
    mine = ref[c, at, rows]
    below, above = pltpu.roll(mine, 1, 1), pltpu.roll(mine, LANES - 1, 1)
    x_minus, x_plus = ref[c, at - 1, rows], ref[c, at + 1, rows]
    z_minus = ref[c, at, first - 1 : first - 1 + count]
    z_plus = ref[c, at, first + 1 : first + 1 + count]
    total = coef[0, g, here] * x_minus + coef[1, g, here] * x_plus
    total = total + (coef[2, g, here] * below + coef[3, g, here] * above)
    total = total + (coef[4, g, here] * z_minus + coef[5, g, here] * z_plus)
    return mine, total, (x_minus, x_plus, below, above, z_minus, z_plus)


def smoother_step(coef, source, target, d0, weight, pieces):
    def body(g, _):
        for first, count in pieces:
            rows = slice(first, first + count)
            for c in range(3):
                _, total, _ = neighbours(coef, source, c, g, first, count)
                target[c, g + 1, rows] = total + weight * d0[c, g + 1, rows]
        return 0

    lax.fori_loop(0, SLABS, body, 0, unroll=UNROLL)
    ghosts(target, range(3), pieces)


def prepare(f, v, ry, ex, visc, coef, inv, diag, d0, d1, d2):
    *shape, leading = smoother_polynomial()

    def place(g, _):
        visc[g + 1, OWN] = v[g]
        return 0

    lax.fori_loop(0, SLABS, place, 0)
    for first, count in OWN_PIECES:
        rows = slice(first, first + count)
        lane = lane_index(count)
        extra = ex[first - 16 : first - 16 + count]
        before = pltpu.roll(visc[SLABS, rows], EY, 1)
        after = pltpu.roll(visc[1, rows], LANES - EY, 1)
        visc[0, rows] = jnp.where(lane < EY, extra, before)
        visc[SLABS + 1, rows] = jnp.where(lane >= LANES - EY, extra, after)
    set_up(f, ry, visc, coef, inv, diag, d0, None, leading, OWN_PIECES)
    smoother_step(coef, d0, d1, d0, shape[-1] / leading, OWN_PIECES)
    smoother_step(coef, d1, d2, d0, shape[-2] / leading, OWN_PIECES)


def solve_local(f, ry, low_z, high_z, *refs):
    kept_refs, refs = refs[7:14], refs[14:]
    visc, coef, inv, diag, d0, d1, d2 = kept_refs
    s0_out, u1_out, s1_out, u2_out, sums, s, p = refs
    z_below, z_above = ~at_start("gz"), ~at_end("gz")
    *shape, leading = smoother_polynomial()
    weights = [x / leading for x in reversed(shape)]
    zero = jnp.zeros((8, LANES), jnp.float32)

    def place(g, _):
        visc[g + 1, 0:8] = zero
        visc[g + 1, 152:160] = zero
        visc[g + 1, 8:16] = kept_if(z_below, low_z[3 * SLABS + g])
        visc[g + 1, 144:152] = kept_if(z_above, high_z[3 * SLABS + g])
        return 0

    lax.fori_loop(0, SLABS, place, 0)
    for g in range(SLABS):
        ninth = (4 * SLABS + g // 8, slice(g % 8, g % 8 + 1))
        visc[g + 1, 7:8] = kept_if(z_below, low_z[ninth])
        visc[g + 1, 152:153] = kept_if(z_above, high_z[ninth])

    def border(ref, which):
        for c in which:
            for g in range(SLABS):
                at = (c, g + 1) if c is not None else (g + 1,)
                ref[(*at, slice(0, 8))] = zero
                ref[(*at, slice(152, 160))] = zero

    for ref in (d0, d1, d2, s):
        border(ref, range(3))
    border(p, [None])
    ghosts(visc, [None], [END_PIECES[0], END_PIECES[-1]])
    set_up(f, ry, visc, coef, inv, diag, d0, (low_z, high_z), leading, END_PIECES)
    smoother_step(coef, d0, d1, d0, weights[0], END_PIECES)
    smoother_step(coef, d1, d2, d0, weights[1], END_PIECES)
    smoother_step(coef, d2, s, d0, weights[2], PIECES)

    def smooth():
        chain = (d0, d1, d2, s)
        for step in range(CHEB - 1):
            smoother_step(coef, chain[step], chain[step + 1], d0, weights[step], PIECES)

    def apply_first(g, _):
        at = g + 1
        for first, count in PIECES:
            rows = slice(first, first + count)
            here = slice(first - 8, first - 8 + count)
            own = slice(first - 16, first - 16 + count)
            is_own = 16 <= first < 144
            flow = None
            for c in range(3):
                mine, total, sides = neighbours(coef, s, c, g, first, count)
                value = diag[g, here] * (mine - total)
                slope = sides[2 * c + 1] - sides[2 * c]
                flow = slope if flow is None else flow + slope
                d0[c, at, rows] = value * inv[g, here] * leading
                if is_own:
                    u1_out[c, g, own] = value
                    s0_out[c, g, own] = mine
            flow = -0.5 * flow
            p[at, rows] = visc[at, rows] * flow
            if is_own:
                u1_out[3, g, own] = flow
        return 0

    lax.fori_loop(0, SLABS, apply_first, 0, unroll=UNROLL)
    ghosts(d0, range(3), PIECES)
    ghosts(p, [None], PIECES)
    smooth()

    def apply_second(g, carry):
        at = g + 1
        lane = lane_index(8)
        y_at = lane & (EY - 1)
        x_at = (lane // EY) * SLABS + g
        own_cells = (x_at >= H) & (x_at < H + BX) & (y_at >= H) & (y_at < H + BY)
        acc = [jnp.zeros((8, LANES), jnp.float32) for _ in range(5)]
        for first, count in OWN_PIECES:
            rows = slice(first, first + count)
            here = slice(first - 8, first - 8 + count)
            own = slice(first - 16, first - 16 + count)
            centre = p[at, rows]
            press = (
                p[at - 1, rows],
                p[at + 1, rows],
                pltpu.roll(centre, 1, 1),
                pltpu.roll(centre, LANES - 1, 1),
                p[at, first - 1 : first - 1 + count],
                p[at, first + 1 : first + 1 + count],
            )
            flow = None
            values = []
            for c in range(3):
                mine, total, sides = neighbours(coef, s, c, g, first, count)
                value = diag[g, here] * (mine - total) + 0.5 * (press[2 * c + 1] - press[2 * c])
                slope = sides[2 * c + 1] - sides[2 * c]
                flow = slope if flow is None else flow + slope
                s1_out[c, g, own] = mine
                values.append(value)
            values.append(-0.5 * flow)
            s1_out[3, g, own] = centre
            parts = [None] * 5
            for c in range(4):
                u2 = values[c]
                u2_out[c, g, own] = u2
                u1 = u1_out[c, g, own]
                pairs = [None, None, u1 * u1, u1 * u2, u2 * u2]
                if c < 3:
                    u0 = f[c, g, own]
                    pairs[0], pairs[1] = u0 * u1, u0 * u2
                for i, pair in enumerate(pairs):
                    if pair is not None:
                        parts[i] = pair if parts[i] is None else parts[i] + pair
            for i in range(5):
                acc[i] = acc[i] + (parts[i][:8] + parts[i][8:])
        return tuple(c + jnp.where(own_cells, a, 0.0) for c, a in zip(carry, acc))

    start = tuple(jnp.zeros((8, LANES), jnp.float32) for _ in range(5))
    acc = lax.fori_loop(0, SLABS, apply_second, start, unroll=UNROLL)
    lane = lane_index(1)
    line = jnp.zeros((1, LANES), jnp.float32)
    for i in range(5):
        both = jnp.sum(jnp.sum(acc[i], axis=0, keepdims=True), axis=1, keepdims=True)
        line = jnp.where(lane == i, both, line)
    sums[...] = line


def combine(gathered, f, s0, u1, s1, u2, solution_to, residual_to, solution_out, residual_out, done):
    line = jnp.sum(gathered[...], axis=0, keepdims=True)
    lane = lane_index(1)

    def entry(i):
        return jnp.sum(jnp.where(lane == i, line, 0.0), axis=1, keepdims=True)

    g01, g02, g11, g12, g22 = (entry(i) for i in range(5))
    lower = g12 / g11
    pivot = g22 - lower * g12
    b = (g02 - lower * g01) / pivot
    a = (g01 - g12 * b) / g11
    copies = []
    for c in range(4):
        for g in range(SLABS):
            if c < 3:
                sol = a * s0[c, g] + b * s1[c, g]
                res = f[c, g] - a * u1[c, g] - b * u2[c, g]
            else:
                sol = b * s1[c, g]
                res = -a * u1[c, g] - b * u2[c, g]
            for out, value in ((solution_out, sol), (residual_out, res)):
                back = value.T
                for k in range(CHUNKS):
                    x = k * SLABS + g - H
                    if 0 <= x < BX:
                        out[c, x] = back[k * EY + H : k * EY + H + BY]
        for i, (out, to) in enumerate(((solution_out, solution_to), (residual_out, residual_to))):
            copies.append(pltpu.make_async_copy(out.at[c], to.at[c], done.at[2 * c + i]))
            copies[-1].start()
    for copy in copies:
        copy.wait()


def struct(*shape):
    return jax.ShapeDtypeStruct(shape, jnp.float32)


def kept(*shape):
    return pltpu.VMEM(shape, jnp.float32)


def call(
    kernel, outs, scratch=(), name=None, mib=16, source=pltpu.VMEM, to=pltpu.VMEM, alias=None, flops=None
):
    result = pl.BlockSpec(memory_space=to)
    given = pl.BlockSpec(memory_space=source)

    def run(*args):
        return pl.pallas_call(
            kernel,
            out_shape=outs,
            in_specs=[given] * len(args),
            out_specs=[result] * len(outs),
            input_output_aliases=alias or {},
            cost_estimate=flops and pl.CostEstimate(flops=flops, bytes_accessed=0, transcendentals=0),
            scratch_shapes=list(scratch),
            compiler_params=pltpu.CompilerParams(vmem_limit_bytes=mib * 1024 * 1024),
            name=name,
        )(*args)

    return run


def swap(tail, head, axis):
    count = lax.axis_size(axis)
    up = [(i, (i + 1) % count) for i in range(count)]
    down = [(j, i) for i, j in up]
    return lax.ppermute(tail, axis, up), lax.ppermute(head, axis, down)


def shards(viscosity, force):
    force, viscosity, tail_x, head_x, tail_y, head_y = call(
        pack_faces,
        [kept(3, BX, BY, BZ), kept(BX, BY, BZ)]
        + [kept(33, BY, BZ)] * 2
        + [kept(FACE_TILES, 8, BZ)] * 2,
        [pltpu.SemaphoreType.DMA((2,))],
        name="pack_faces",
        source=pltpu.HBM,
    )(*(pltpu.with_memory_space_constraint(x, pltpu.HBM) for x in (force, viscosity)))
    low_y, high_y = swap(tail_y, head_y, "gy")
    low_x, high_x = swap(tail_x, head_x, "gx")
    tail, head = call(pack_corners, [kept(CORNER_TILES, 8, BZ)] * 2, name="pack_corners")(
        low_x, high_x
    )
    low_c, high_c = swap(tail, head, "gy")
    field = (SLABS, BZ, LANES)
    f, v, ry, ex, tail, head = call(
        to_lanes,
        [kept(3, *field), kept(*field), kept(*field), kept(BZ, LANES)]
        + [kept(ZTILES, 8, LANES)] * 2,
        name="to_lanes",
    )(force, viscosity, low_x, high_x, low_y, high_y, low_c, high_c)
    low_z, high_z = swap(tail, head, "gz")
    ghosted = (SLABS + 2, ROWS, LANES)
    plain = (SLABS, EZ, LANES)
    state_shapes = [kept(*ghosted), kept(6, *plain), kept(*plain), kept(*plain)]
    state_shapes += [kept(3, *ghosted)] * 3
    state = call(prepare, state_shapes, name="prepare", flops=120 * EX * EY * BZ)(f, v, ry, ex)
    *_, s0, u1, s1, u2, sums = call(
        solve_local,
        state_shapes
        + [kept(3, *field), kept(4, *field), kept(4, *field), kept(4, *field), kept(1, LANES)],
        [pltpu.VMEM((3, *ghosted), jnp.float32), pltpu.VMEM(ghosted, jnp.float32)],
        name="solve_local",
        alias={4 + i: i for i in range(7)},
    )(f, ry, low_z, high_z, *state)
    devices = lax.axis_size(AXES)
    rows = jnp.broadcast_to(sums[None], (devices, 1, LANES))
    gathered = lax.all_to_all(rows, AXES, 0, 0).reshape(devices, LANES)
    block = struct(4, BX, BY, BZ)
    whole = pltpu.VMEM((4, BX, BY, BZ), jnp.float32)
    return tuple(
        call(
            combine,
            [block, block],
            [whole, whole, pltpu.SemaphoreType.DMA((8,))],
            name="combine",
            to=pltpu.HBM,
        )(gathered, f, s0, u1, s1, u2)
    )


def solution(mesh):
    return jax.shard_map(
        shards,
        mesh=mesh,
        in_specs=(P("gx", "gy", "gz"), P(None, "gx", "gy", "gz")),
        out_specs=(P(None, "gx", "gy", "gz"), P(None, "gx", "gy", "gz")),
        check_vma=False,
    )
```

```python
import jax
import jax.numpy as jnp
from jax import lax
from jax.experimental import pallas as pl
from jax.experimental.pallas import tpu as pltpu
from jax.sharding import PartitionSpec as P


CHEB = 4
LOW_EDGE = 0.25
HIGH_EDGE = 2.0
MIDDLE = 0.5 * (HIGH_EDGE + LOW_EDGE)
HALF = 0.5 * (HIGH_EDGE - LOW_EDGE)
AXES = ("gx", "gy", "gz")

BX, BY, BZ, H = 32, 16, 128, 8
EX, EY, EZ = BX + 2 * H, BY + 2 * H, BZ + 2 * H
CHUNKS = 4
UNROLL = 12
SLABS = EX // CHUNKS
LANES = CHUNKS * EY
ROWS = EZ + 16
ZTILES = 4 * SLABS + 2
OWN = slice(16, 16 + BZ)
PIECES = [(8, 8)] + [(16 + 16 * i, 16) for i in range(8)] + [(144, 8)]
OWN_PIECES = PIECES[1:-1]
END_PIECES = [(8, 8), (16, 8), (136, 8), (144, 8)]


def smoother_polynomial():
    def minus_operator(p):
        return [high - low for low, high in zip(p + [0.0], [0.0] + p)]

    def plus(p, q):
        size = max(len(p), len(q))
        return [x + y for x, y in zip(p + [0.0] * (size - len(p)), q + [0.0] * (size - len(q)))]

    scaled = MIDDLE / HALF
    now = 1.0 / scaled
    update, remainder = [1.0 / MIDDLE], [1.0]
    result = update
    for _ in range(CHEB - 1):
        remainder = plus(remainder, minus_operator(update))
        following = 1.0 / (2.0 * scaled - now)
        update = plus(
            [following * now * x for x in update], [2.0 * following / HALF * x for x in remainder]
        )
        result = plus(result, update)
        now = following
    return result


def shared_tiles(reach):
    def at(side, far):
        return H - far if side == 0 else H + BX - 1 + far

    tiles = []
    for side in (0, 1):
        for far in range(1, H + 1):
            rows, other = reach - far, 2 * reach - 8 - far
            if rows == 8 or far < other:
                tiles.append((at(side, far), rows, None if rows == 8 else at(side, other)))
    half = reach - 4
    tiles.append((at(0, half), 4, at(1, half)))
    return tiles


FORCE_TILES = shared_tiles(8)
VISC_TILES = shared_tiles(9)
FACE_TILES = 4 * BX + BX // 8
CORNER_TILES = 3 * len(FORCE_TILES) + len(VISC_TILES)


def corner_places(c):
    places = {}
    for i, (first, rows, second) in enumerate(FORCE_TILES if c < 3 else VISC_TILES):
        at = c * len(FORCE_TILES) + i
        places[first] = (at, rows, False)
        if second is not None:
            places[second] = (at, rows, True)
    return places


def kept_if(condition, value):
    return jnp.where(condition, value, 0.0)


def at_start(axis):
    return lax.axis_index(axis) == 0


def at_end(axis):
    return lax.axis_index(axis) == lax.axis_size(axis) - 1


def at_even(axis):
    return lax.axis_index(axis) % 2 == 0


def pack_faces(force_in, visc_in, force, visc, tail_x, head_x, first_y, second_y, arrived):
    even = at_even("gy")
    copies = [
        pltpu.make_async_copy(visc_in, visc, arrived.at[0]),
        pltpu.make_async_copy(force_in, force, arrived.at[1]),
    ]
    for copy in copies:
        copy.start()
    copies[0].wait()
    tail_x[24:] = visc[BX - 9 :]
    head_x[24:] = visc[:9]
    top, bottom = (BY - 8, BY - 9), (0, 8)
    starts = [
        [jnp.where(even, one, two) for one, two in zip(near, far)]
        for near, far in ((top, bottom), (bottom, top))
    ]
    for out, (first, ninth) in zip((first_y, second_y), starts):
        rows = pl.ds(pl.multiple_of(first, 8), 8)
        out[3 * BX : 4 * BX] = visc[:, rows, :]
        for x in range(BX):
            out[4 * BX + x // 8, x % 8 : x % 8 + 1, :] = visc[x, pl.ds(ninth, 1), :]
    copies[1].wait()
    for c in range(3):
        tail_x[c * 8 : c * 8 + 8] = force[c, BX - 8 :]
        head_x[c * 8 : c * 8 + 8] = force[c, :8]
        for out, (first, _) in zip((first_y, second_y), starts):
            out[c * BX : c * BX + BX] = force[c, :, pl.ds(pl.multiple_of(first, 8), 8), :]


def pack_corners(low_x, high_x, tail, head):
    row = lax.broadcasted_iota(jnp.int32, (8, BZ), 0)
    from_below, from_above = ~at_start("gx"), ~at_end("gx")
    for out, up in ((tail, True), (head, False)):
        first = BY - 8 if up else 0
        rows = slice(first, first + 8)

        def tile(c, at):
            if at < H:
                if c < 3:
                    return low_x[c * 8 + at, rows, :]
                return kept_if(from_below, low_x[25 + at, rows, :])
            at = at - H - BX
            return high_x[c * 8 + at, rows, :] if c < 3 else kept_if(from_above, high_x[24 + at, rows, :])

        for c in range(4):
            for i, (one, count, two) in enumerate(FORCE_TILES if c < 3 else VISC_TILES):
                value = tile(c, one)
                if two is not None:
                    other = tile(c, two)
                    if up:
                        value = jnp.where(row >= 8 - count, value, pltpu.roll(other, 8 - count, 0))
                    else:
                        value = jnp.where(row < count, value, pltpu.roll(other, count, 0))
                out[c * len(FORCE_TILES) + i] = value


def to_lanes(
    force, visc, low_x, high_x, first_y, second_y, low_c, high_c,
    f_out, v_out, ry_out, ex_out, tail, head,
):
    x_below, x_above = ~at_start("gx"), ~at_end("gx")
    y_below, y_above = ~at_start("gy"), ~at_end("gy")
    places = [corner_places(c) for c in range(4)]
    even = at_even("gy")

    def beside(*at):
        one, two = first_y[at], second_y[at]
        return jnp.where(even, two, one), jnp.where(even, one, two)

    def rows_of(c, at):
        x = at - H
        if x < 0:
            middle = low_x[c * 8 + at] if c < 3 else kept_if(x_below, low_x[25 + at])
        elif x >= BX:
            middle = high_x[c * 8 + x - BX] if c < 3 else kept_if(x_above, high_x[24 + x - BX])
        else:
            middle = force[c, x] if c < 3 else visc[x]
        if 0 <= x < BX:
            lower, upper = beside(c * BX + x)
        elif at in places[c]:
            where, count, second = places[c][at]
            lower, upper = low_c[where], high_c[where]
            if second:
                lower, upper = pltpu.roll(lower, count, 0), pltpu.roll(upper, 8 - count, 0)
        else:
            lower = upper = jnp.zeros((8, BZ), jnp.float32)
        if c == 3:
            lower, upper = kept_if(y_below, lower), kept_if(y_above, upper)
        return [lower, middle, upper]

    for c in range(4):
        for g in range(SLABS):
            parts = []
            for k in range(CHUNKS):
                parts += rows_of(c, k * SLABS + g)
            block = jnp.concatenate(parts, axis=0).T
            if c < 3:
                f_out[c, g] = block
            else:
                v_out[g] = block
                tail[4 * SLABS + g // 8, g % 8 : g % 8 + 1, :] = block[BZ - 9 : BZ - 8]
                head[4 * SLABS + g // 8, g % 8 : g % 8 + 1, :] = block[8:9]
            tail[c * SLABS + g] = block[BZ - 8 :]
            head[c * SLABS + g] = block[:8]
    for out in (tail, head):
        out[ZTILES - 1, SLABS - 8 :, :] = jnp.zeros((16 - SLABS, LANES), jnp.float32)
    nothing = jnp.zeros((EY - 2, BZ), jnp.float32)
    for g in range(SLABS):
        parts = []
        for k in range(CHUNKS):
            x = k * SLABS + g - H
            if 0 <= x < BX:
                at = 4 * BX + x // 8
                lower, upper = beside(at, slice(x % 8, x % 8 + 1))
                lower, upper = kept_if(y_below, lower), kept_if(y_above, upper)
            else:
                lower = upper = jnp.zeros((1, BZ), jnp.float32)
            parts += [lower, nothing, upper]
        ry_out[g] = jnp.concatenate(parts, axis=0).T
    side = jnp.zeros((8, BZ), jnp.float32)
    between = jnp.zeros((2 * EY, BZ), jnp.float32)
    ex_out[...] = jnp.concatenate(
        [
            side, kept_if(x_below, low_x[24]), side, between,
            side, kept_if(x_above, high_x[32]), side,
        ],
        axis=0,
    ).T


def lane_index(rows):
    return lax.broadcasted_iota(jnp.int32, (rows, LANES), 1)


def ghosts(ref, which, pieces):
    for c in which:
        for first, count in pieces:
            rows = slice(first, first + count)
            pre = (c,) if c is not None else ()
            ref[(*pre, 0, rows)] = pltpu.roll(ref[(*pre, SLABS, rows)], EY, 1)
            ref[(*pre, SLABS + 1, rows)] = pltpu.roll(ref[(*pre, 1, rows)], LANES - EY, 1)


def set_up(f, ry, visc, coef, inv, diag, d0, halo, leading, pieces):
    def body(g, _):
        at = g + 1
        for first, count in pieces:
            rows = slice(first, first + count)
            here = slice(first - 8, first - 8 + count)
            lane = lane_index(count)
            y_at = lane & (EY - 1)
            mine = visc[at, rows]
            below, above = pltpu.roll(mine, 1, 1), pltpu.roll(mine, LANES - 1, 1)
            if 16 <= first < 144:
                extra = ry[g, first - 16 : first - 16 + count]
                below = jnp.where(y_at == 0, extra, below)
                above = jnp.where(y_at == EY - 1, extra, above)
            x_plus = 0.5 * (mine + visc[at + 1, rows])
            x_minus = 0.5 * (mine + visc[at - 1, rows])
            y_plus = 0.5 * (mine + above)
            y_minus = 0.5 * (mine + below)
            z_plus = 0.5 * (mine + visc[at, first + 1 : first + 1 + count])
            z_minus = 0.5 * (mine + visc[at, first - 1 : first - 1 + count])
            total = x_plus + x_minus + y_plus + y_minus + z_plus + z_minus
            inside = mine > 0.0
            inverse = jnp.where(inside, 1.0 / jnp.where(inside, total, 1.0), 0.0)
            inv[g, here] = inverse
            diag[g, here] = total
            for i, face in enumerate((x_minus, x_plus, y_minus, y_plus, z_minus, z_plus)):
                coef[i, g, here] = face * inverse
            for c in range(3):
                if first == 8:
                    value = halo[0][c * SLABS + g]
                elif first == 144:
                    value = halo[1][c * SLABS + g]
                else:
                    value = f[c, g, first - 16 : first - 16 + count]
                d0[c, at, rows] = value * inverse * leading
        return 0

    lax.fori_loop(0, SLABS, body, 0, unroll=UNROLL)
    ghosts(d0, range(3), pieces)


def neighbours(coef, ref, c, g, first, count):
    at = g + 1
    rows = slice(first, first + count)
    here = slice(first - 8, first - 8 + count)
    mine = ref[c, at, rows]
    below, above = pltpu.roll(mine, 1, 1), pltpu.roll(mine, LANES - 1, 1)
    x_minus, x_plus = ref[c, at - 1, rows], ref[c, at + 1, rows]
    z_minus = ref[c, at, first - 1 : first - 1 + count]
    z_plus = ref[c, at, first + 1 : first + 1 + count]
    total = coef[0, g, here] * x_minus + coef[1, g, here] * x_plus
    total = total + (coef[2, g, here] * below + coef[3, g, here] * above)
    total = total + (coef[4, g, here] * z_minus + coef[5, g, here] * z_plus)
    return mine, total, (x_minus, x_plus, below, above, z_minus, z_plus)


def smoother_step(coef, source, target, d0, weight, pieces):
    def body(g, _):
        for first, count in pieces:
            rows = slice(first, first + count)
            for c in range(3):
                _, total, _ = neighbours(coef, source, c, g, first, count)
                target[c, g + 1, rows] = total + weight * d0[c, g + 1, rows]
        return 0

    lax.fori_loop(0, SLABS, body, 0, unroll=UNROLL)
    ghosts(target, range(3), pieces)


def prepare(f, v, ry, ex, visc, coef, inv, diag, d0, d1, d2):
    *shape, leading = smoother_polynomial()

    def place(g, _):
        visc[g + 1, OWN] = v[g]
        return 0

    lax.fori_loop(0, SLABS, place, 0)
    for first, count in OWN_PIECES:
        rows = slice(first, first + count)
        lane = lane_index(count)
        extra = ex[first - 16 : first - 16 + count]
        before = pltpu.roll(visc[SLABS, rows], EY, 1)
        after = pltpu.roll(visc[1, rows], LANES - EY, 1)
        visc[0, rows] = jnp.where(lane < EY, extra, before)
        visc[SLABS + 1, rows] = jnp.where(lane >= LANES - EY, extra, after)
    set_up(f, ry, visc, coef, inv, diag, d0, None, leading, OWN_PIECES)
    smoother_step(coef, d0, d1, d0, shape[-1] / leading, OWN_PIECES)
    smoother_step(coef, d1, d2, d0, shape[-2] / leading, OWN_PIECES)


def solve_local(f, ry, low_z, high_z, *refs):
    kept_refs, refs = refs[7:14], refs[14:]
    visc, coef, inv, diag, d0, d1, d2 = kept_refs
    s0_out, u1_out, s1_out, u2_out, sums, s, p = refs
    z_below, z_above = ~at_start("gz"), ~at_end("gz")
    *shape, leading = smoother_polynomial()
    weights = [x / leading for x in reversed(shape)]
    zero = jnp.zeros((8, LANES), jnp.float32)

    def place(g, _):
        visc[g + 1, 0:8] = zero
        visc[g + 1, 152:160] = zero
        visc[g + 1, 8:16] = kept_if(z_below, low_z[3 * SLABS + g])
        visc[g + 1, 144:152] = kept_if(z_above, high_z[3 * SLABS + g])
        return 0

    lax.fori_loop(0, SLABS, place, 0)
    for g in range(SLABS):
        ninth = (4 * SLABS + g // 8, slice(g % 8, g % 8 + 1))
        visc[g + 1, 7:8] = kept_if(z_below, low_z[ninth])
        visc[g + 1, 152:153] = kept_if(z_above, high_z[ninth])

    def border(ref, which):
        for c in which:
            for g in range(SLABS):
                at = (c, g + 1) if c is not None else (g + 1,)
                ref[(*at, slice(0, 8))] = zero
                ref[(*at, slice(152, 160))] = zero

    for ref in (d0, d1, d2, s):
        border(ref, range(3))
    border(p, [None])
    ghosts(visc, [None], [END_PIECES[0], END_PIECES[-1]])
    set_up(f, ry, visc, coef, inv, diag, d0, (low_z, high_z), leading, END_PIECES)
    smoother_step(coef, d0, d1, d0, weights[0], END_PIECES)
    smoother_step(coef, d1, d2, d0, weights[1], END_PIECES)
    smoother_step(coef, d2, s, d0, weights[2], PIECES)

    def smooth():
        chain = (d0, d1, d2, s)
        for step in range(CHEB - 1):
            smoother_step(coef, chain[step], chain[step + 1], d0, weights[step], PIECES)

    def apply_first(g, _):
        at = g + 1
        for first, count in PIECES:
            rows = slice(first, first + count)
            here = slice(first - 8, first - 8 + count)
            own = slice(first - 16, first - 16 + count)
            is_own = 16 <= first < 144
            flow = None
            for c in range(3):
                mine, total, sides = neighbours(coef, s, c, g, first, count)
                value = diag[g, here] * (mine - total)
                slope = sides[2 * c + 1] - sides[2 * c]
                flow = slope if flow is None else flow + slope
                d0[c, at, rows] = value * inv[g, here] * leading
                if is_own:
                    u1_out[c, g, own] = value
                    s0_out[c, g, own] = mine
            flow = -0.5 * flow
            p[at, rows] = visc[at, rows] * flow
            if is_own:
                u1_out[3, g, own] = flow
        return 0

    lax.fori_loop(0, SLABS, apply_first, 0, unroll=UNROLL)
    ghosts(d0, range(3), PIECES)
    ghosts(p, [None], PIECES)
    smooth()

    def apply_second(g, carry):
        at = g + 1
        lane = lane_index(8)
        y_at = lane & (EY - 1)
        x_at = (lane // EY) * SLABS + g
        own_cells = (x_at >= H) & (x_at < H + BX) & (y_at >= H) & (y_at < H + BY)
        acc = [jnp.zeros((8, LANES), jnp.float32) for _ in range(5)]
        for first, count in OWN_PIECES:
            rows = slice(first, first + count)
            here = slice(first - 8, first - 8 + count)
            own = slice(first - 16, first - 16 + count)
            centre = p[at, rows]
            press = (
                p[at - 1, rows],
                p[at + 1, rows],
                pltpu.roll(centre, 1, 1),
                pltpu.roll(centre, LANES - 1, 1),
                p[at, first - 1 : first - 1 + count],
                p[at, first + 1 : first + 1 + count],
            )
            flow = None
            values = []
            for c in range(3):
                mine, total, sides = neighbours(coef, s, c, g, first, count)
                value = diag[g, here] * (mine - total) + 0.5 * (press[2 * c + 1] - press[2 * c])
                slope = sides[2 * c + 1] - sides[2 * c]
                flow = slope if flow is None else flow + slope
                s1_out[c, g, own] = mine
                values.append(value)
            values.append(-0.5 * flow)
            s1_out[3, g, own] = centre
            parts = [None] * 5
            for c in range(4):
                u2 = values[c]
                u2_out[c, g, own] = u2
                u1 = u1_out[c, g, own]
                pairs = [None, None, u1 * u1, u1 * u2, u2 * u2]
                if c < 3:
                    u0 = f[c, g, own]
                    pairs[0], pairs[1] = u0 * u1, u0 * u2
                for i, pair in enumerate(pairs):
                    if pair is not None:
                        parts[i] = pair if parts[i] is None else parts[i] + pair
            for i in range(5):
                acc[i] = acc[i] + (parts[i][:8] + parts[i][8:])
        return tuple(c + jnp.where(own_cells, a, 0.0) for c, a in zip(carry, acc))

    start = tuple(jnp.zeros((8, LANES), jnp.float32) for _ in range(5))
    acc = lax.fori_loop(0, SLABS, apply_second, start, unroll=UNROLL)
    lane = lane_index(1)
    line = jnp.zeros((1, LANES), jnp.float32)
    for i in range(5):
        both = jnp.sum(jnp.sum(acc[i], axis=0, keepdims=True), axis=1, keepdims=True)
        line = jnp.where(lane == i, both, line)
    sums[...] = line


def combine(gathered, f, s0, u1, s1, u2, solution_to, residual_to, solution_out, residual_out, done):
    line = jnp.sum(gathered[...], axis=0, keepdims=True)
    lane = lane_index(1)

    def entry(i):
        return jnp.sum(jnp.where(lane == i, line, 0.0), axis=1, keepdims=True)

    g01, g02, g11, g12, g22 = (entry(i) for i in range(5))
    lower = g12 / g11
    pivot = g22 - lower * g12
    b = (g02 - lower * g01) / pivot
    a = (g01 - g12 * b) / g11
    copies = []
    for c in range(4):
        for g in range(SLABS):
            if c < 3:
                sol = a * s0[c, g] + b * s1[c, g]
                res = f[c, g] - a * u1[c, g] - b * u2[c, g]
            else:
                sol = b * s1[c, g]
                res = -a * u1[c, g] - b * u2[c, g]
            for out, value in ((solution_out, sol), (residual_out, res)):
                back = value.T
                for k in range(CHUNKS):
                    x = k * SLABS + g - H
                    if 0 <= x < BX:
                        out[c, x] = back[k * EY + H : k * EY + H + BY]
        for i, (out, to) in enumerate(((solution_out, solution_to), (residual_out, residual_to))):
            copies.append(pltpu.make_async_copy(out.at[c], to.at[c], done.at[2 * c + i]))
            copies[-1].start()
    for copy in copies:
        copy.wait()


def struct(*shape):
    return jax.ShapeDtypeStruct(shape, jnp.float32)


def kept(*shape):
    return pltpu.VMEM(shape, jnp.float32)


def call(
    kernel, outs, scratch=(), mib=16, source=pltpu.VMEM, to=pltpu.VMEM, alias=None, flops=None
):
    result = pl.BlockSpec(memory_space=to)
    given = pl.BlockSpec(memory_space=source)

    def run(*args):
        return pl.pallas_call(
            kernel,
            out_shape=outs,
            in_specs=[given] * len(args),
            out_specs=[result] * len(outs),
            input_output_aliases=alias or {},
            cost_estimate=flops and pl.CostEstimate(flops=flops, bytes_accessed=0, transcendentals=0),
            scratch_shapes=list(scratch),
            compiler_params=pltpu.CompilerParams(vmem_limit_bytes=mib * 1024 * 1024),
        )(*args)

    return run


def swap(tail, head, axis):
    count = lax.axis_size(axis)
    up = [(i, (i + 1) % count) for i in range(count)]
    down = [(j, i) for i, j in up]
    low = lax.ppermute(tail, axis, up)
    high = lax.ppermute(head, axis, down)
    return low, high


def swap_pairs(first, second, axis):
    count = lax.axis_size(axis)
    pairs = [[], []]
    for i in range(count):
        pairs[i % 2] += [(i, (i + 1) % count), ((i + 1) % count, i)]
    first = lax.ppermute(first, axis, pairs[0])
    second = lax.ppermute(second, axis, pairs[1])
    return first, second


def shards(viscosity, force):
    force, viscosity, tail_x, head_x, first_y, second_y = call(
        pack_faces,
        [kept(3, BX, BY, BZ), kept(BX, BY, BZ)]
        + [kept(33, BY, BZ)] * 2
        + [kept(FACE_TILES, 8, BZ)] * 2,
        [pltpu.SemaphoreType.DMA((2,))],
        source=pltpu.HBM,
    )(*(pltpu.with_memory_space_constraint(x, pltpu.HBM) for x in (force, viscosity)))
    first_y, second_y = swap_pairs(first_y, second_y, "gy")
    low_x, high_x = swap(tail_x, head_x, "gx")
    tail, head = call(pack_corners, [kept(CORNER_TILES, 8, BZ)] * 2)(low_x, high_x)
    low_c, high_c = swap(tail, head, "gy")
    field = (SLABS, BZ, LANES)
    f, v, ry, ex, tail, head = call(
        to_lanes,
        [kept(3, *field), kept(*field), kept(*field), kept(BZ, LANES)]
        + [kept(ZTILES, 8, LANES)] * 2,
    )(force, viscosity, low_x, high_x, first_y, second_y, low_c, high_c)
    low_z, high_z = swap(tail, head, "gz")
    ghosted = (SLABS + 2, ROWS, LANES)
    plain = (SLABS, EZ, LANES)
    state_shapes = [kept(*ghosted), kept(6, *plain), kept(*plain), kept(*plain)]
    state_shapes += [kept(3, *ghosted)] * 3
    state = call(prepare, state_shapes, flops=120 * EX * EY * BZ)(f, v, ry, ex)
    *_, s0, u1, s1, u2, sums = call(
        solve_local,
        state_shapes
        + [kept(3, *field), kept(4, *field), kept(4, *field), kept(4, *field), kept(1, LANES)],
        [pltpu.VMEM((3, *ghosted), jnp.float32), pltpu.VMEM(ghosted, jnp.float32)],
        alias={4 + i: i for i in range(7)},
    )(f, ry, low_z, high_z, *state)
    devices = lax.axis_size(AXES)
    rows = jnp.broadcast_to(sums[None], (devices, 1, LANES))
    gathered = lax.all_to_all(rows, AXES, 0, 0).reshape(devices, LANES)
    block = struct(4, BX, BY, BZ)
    whole = pltpu.VMEM((4, BX, BY, BZ), jnp.float32)
    return tuple(
        call(
            combine, [block, block], [whole, whole, pltpu.SemaphoreType.DMA((8,))], to=pltpu.HBM
        )(gathered, f, s0, u1, s1, u2)
    )


def solution(mesh):
    return jax.shard_map(
        shards,
        mesh=mesh,
        in_specs=(P("gx", "gy", "gz"), P(None, "gx", "gy", "gz")),
        out_specs=(P(None, "gx", "gy", "gz"), P(None, "gx", "gy", "gz")),
        check_vma=False,
    )
```
